32 devices in a mesh: replica: 2 (over core), model: 4 (over y, x), copy: 4 (over z).
Axes of the slice: x: 2, y: 2, z: 4, core: 2. Of those that a mesh axis runs over, the one named last changes fastest.
Arguments:
- slope_up: bfloat16 [8, 1280, 5120], P(('copy', 'replica'), None, 'model'), parts along dimension 0, may hold values from -0.875 to 0.875
- slope_down: bfloat16 [8, 5120, 1280], P(('copy', 'replica'), 'model'), parts along dimension 0, may hold values from -0.875 to 0.875
- slope_norm: bfloat16 [8, 1280], P(('copy', 'replica')), parts along dimension 0, may hold values from -8 to 8
- param_up: float32 [5120, 5120], P(('copy', 'replica'), 'model'), parts along dimension 0, may hold values from -0.25 to 0.25
- param_down: float32 [20480, 1280], P(('copy', 'model'), 'replica'), parts along dimension 0, may hold values from -0.125 to 0.125
- param_norm: float32 [5120], P(('copy', 'replica')), parts along dimension 0, may hold values from 0.25 to 1.75
Outputs:
- half_up: bfloat16 [5120, 5120], P('copy', 'model'), parts along dimension 0
- half_down: bfloat16 [20480, 1280], P(('copy', 'model')), parts along dimension 0
- half_norm: bfloat16 [5120], P('copy'), parts along dimension 0
- next_up: float32 [5120, 5120], P(('copy', 'replica'), 'model'), parts along dimension 0
- next_down: float32 [20480, 1280], P(('copy', 'model'), 'replica'), parts along dimension 0
- next_norm: float32 [5120], P(('copy', 'replica')), parts along dimension 0
The draws below stay inside these ranges and needn't reach their ends.
There are 4 independent parts, one for each index of `copy`. The reference program is written for one: setup_inputs(seed, part) draws one part's arguments, and reference() takes and returns one part's arrays. A program takes and returns all parts, laid end to end along the dimension named above; each array names one. Nothing has to cross between parts.
All inputs are finite; a program needn't handle non-finite values.
Results may differ from the reference program's by a relative error of at most 0.011.
Values may be sent and summed in bfloat16 or wider, within the bound.
A program may use at most 128 MiB of HBM per device.

```python
import jax
import jax.numpy as jnp
from jax import lax

WIDTH = 1280
INNER = 5120
REPLICAS = 2


def spiked(drawn, rng, source, target, shards_of, factor):
    def block_of(dim):
        return (jnp.arange(drawn.shape[dim]) // (drawn.shape[dim] // shards_of)).reshape((-1,) + (1,) * (drawn.ndim - 1 - dim))

    first = jax.random.permutation(rng, shards_of)[block_of(target)]
    other_side = (block_of(target) + shards_of // 2) % shards_of
    return jnp.where((block_of(source) == first) | (block_of(source) == other_side), factor * drawn, drawn)


def level_of(stream_key, shape, cuts, least, top_value):
    level = 1.0
    for dim, parts in cuts:
        steps = jax.random.uniform(jax.random.fold_in(jax.random.fold_in(stream_key, 6), dim), (parts,), jnp.float32, least / len(cuts), top_value / len(cuts))
        level = level * jnp.repeat(jnp.exp(steps), shape[dim] // parts).reshape((-1,) + (1,) * (len(shape) - 1 - dim))
    return level


def noise_with(own_key, dims, spread, limit, pieces, heavy, dtype=jnp.bfloat16):
    array = spread * jax.random.normal(own_key, dims, jnp.float32)
    if pieces:
        array = array * level_of(own_key, dims, pieces, -0.22, 0.18)
    return jnp.clip(spiked(array, jax.random.fold_in(own_key, 3), *heavy), -limit, limit).astype(dtype)


def setup_inputs(seed: int = 0, part: int = 0) -> dict:
    key_of = jax.random.split(jax.random.key(seed), 7)
    part_keys = jax.random.split(jax.random.fold_in(key_of[6], part), 7)
    return {
        "slope_up": noise_with(part_keys[0], (REPLICAS, WIDTH, INNER), 0.1, 0.875, ((0, 2), (2, 4)), (0, 1, 2, 2.0)),
        "slope_down": noise_with(part_keys[1], (REPLICAS, INNER, WIDTH), 0.1, 0.875, ((0, 2), (1, 4)), (0, 2, 2, 2.0)),
        "slope_norm": noise_with(part_keys[2], (REPLICAS, WIDTH), 1.0, 8.0, ((0, 2),), (0, 1, 2, 2.0)),
        "param_up": noise_with(part_keys[3], (WIDTH, INNER), WIDTH ** -0.5, 0.25, ((0, 2), (1, 4)), (1, 0, 4, 2.0), jnp.float32),
        "param_down": noise_with(part_keys[4], (INNER, WIDTH), INNER ** -0.5, 0.125, ((0, 4), (1, 2)), (0, 1, 4, 2.0), jnp.float32),
        "param_norm": jnp.clip(1.0 + 0.15 * jax.random.normal(part_keys[5], (WIDTH,), jnp.float32), 0.25, 1.75),
    }


learn_rate = 0.5

def reference(slope_up, slope_down, slope_norm, param_up, param_down, param_norm):
    mean_up = lax.optimization_barrier(jnp.sum(slope_up.astype(jnp.float32), axis=0)) * REPLICAS ** (-0.5)
    mean_down = lax.optimization_barrier(jnp.sum(slope_down.astype(jnp.float32), axis=0)) * REPLICAS ** (-0.5)
    mean_norm = lax.optimization_barrier(jnp.sum(slope_norm.astype(jnp.float32), axis=0)) * REPLICAS ** (-0.5)
    ratio_up = jnp.sqrt(lax.optimization_barrier(jnp.sum(param_up * param_up, axis=1, keepdims=True))) * lax.rsqrt(lax.optimization_barrier(jnp.sum(mean_up * mean_up, axis=1, keepdims=True)) + 1e-06)
    mean_up = mean_up * ratio_up
    ratio_down = jnp.sqrt(lax.optimization_barrier(jnp.sum(param_down * param_down, axis=0, keepdims=True))) * lax.rsqrt(lax.optimization_barrier(jnp.sum(mean_down * mean_down, axis=0, keepdims=True)) + 1e-06)
    mean_down = mean_down * ratio_down
    next_up = param_up - learn_rate * mean_up
    next_down = param_down - learn_rate * mean_down
    next_norm = param_norm - learn_rate * mean_norm
    half_up = next_up.astype(jnp.bfloat16)
    half_down = next_down.astype(jnp.bfloat16)
    half_norm = next_norm.astype(jnp.bfloat16)
    return (half_up, half_down, half_norm, next_up, next_down, next_norm)
```

```python
import functools

import jax
import jax.numpy as jnp
from jax import lax
from jax.experimental import pallas as pl
from jax.experimental.pallas import tpu as pltpu
from jax.sharding import PartitionSpec as P

learn_rate = 0.5


def shards(slope_up, slope_down, slope_norm, param_up, param_down, param_norm):
    mean_up, mean_down = (
        lax.psum_scatter(
            slope_up[0].astype(jnp.float32).astype(jnp.bfloat16),
            "replica",
            scatter_dimension=0,
            tiled=True,
        ).astype(jnp.float32),
        lax.psum_scatter(
            slope_down[0].astype(jnp.float32).astype(jnp.bfloat16),
            "replica",
            scatter_dimension=1,
            tiled=True,
        ).astype(jnp.float32),
    )
    whole_norm = lax.psum(slope_norm[0].astype(jnp.float32), "replica")
    place = lax.axis_index("replica")
    mean_norm = lax.dynamic_slice_in_dim(
        whole_norm, place * param_norm.shape[0], param_norm.shape[0]
    )
    mean_rate = lax.axis_size("replica") ** (-0.5)
    mean_up = mean_up * mean_rate
    mean_down = mean_down * mean_rate
    mean_norm = mean_norm * mean_rate
    own_up, own_down, slope_up_norm, slope_down_norm = lax.psum(
        (
            jnp.sum(param_up * param_up, axis=1, keepdims=True),
            jnp.sum(param_down * param_down, axis=0, keepdims=True),
            jnp.sum(mean_up * mean_up, axis=1, keepdims=True),
            jnp.sum(mean_down * mean_down, axis=0, keepdims=True),
        ),
        "model",
    )
    mean_up = mean_up * (jnp.sqrt(own_up) * lax.rsqrt(slope_up_norm + 1e-06))
    mean_down = mean_down * (jnp.sqrt(own_down) * lax.rsqrt(slope_down_norm + 1e-06))
    next_up = param_up - learn_rate * mean_up
    next_down = param_down - learn_rate * mean_down
    next_norm = param_norm - learn_rate * mean_norm
    half_up, half_down, half_norm = (
        lax.all_gather(next_up.astype(jnp.bfloat16), "replica", axis=0, tiled=True),
        lax.all_gather(next_down.astype(jnp.bfloat16), "replica", axis=1, tiled=True),
        lax.all_gather(next_norm.astype(jnp.bfloat16), "replica", axis=0, tiled=True),
    )
    return (half_up, half_down, half_norm, next_up, next_down, next_norm)


MESH = pl.DeviceIdType.MESH
LANES = 128
ROWS = 32
AHEAD = 6


def update_kernel(
    replicas,
    models,
    slope_up,
    slope_down,
    slope_norm,
    param_up,
    param_down,
    param_norm,
    half_up,
    half_down,
    half_norm,
    next_up,
    next_down,
    next_norm,
    own_up,
    peer_up,
    own_down,
    peer_down,
    own_vec,
    peer_vec,
    own_gain,
    peer_gain,
    sum_vec,
    part,
    got,
    piece,
    got_piece,
    square,
    spread,
    load_sem,
    pair_send,
    pair_recv,
    norm_send,
    norm_recv,
    piece_send,
    piece_recv,
    pair_ready,
    model_ready,
):
    me = lax.axis_index("replica")
    other = 1 - me
    spot = lax.axis_index("model")
    share, inner = param_up.shape
    depth = param_down.shape[0]
    up_chunks = share // LANES
    down_chunks = share // LANES
    down_rows = 4 * ROWS
    mine = pl.multiple_of(me * share, LANES)
    theirs = pl.multiple_of(other * share, LANES)
    rate = replicas ** (-0.5)
    f32 = jnp.float32

    loads = {}

    def load(name, source, target):
        copy = pltpu.make_async_copy(source, target, load_sem.at[len(loads)])
        copy.start()
        loads[name] = copy

    pairs = {}

    def push(name, source, target):
        copy = pltpu.make_async_remote_copy(
            source,
            target,
            pair_send.at[len(pairs)],
            pair_recv.at[len(pairs)],
            device_id={"replica": other},
            device_id_type=MESH,
        )
        copy.start()
        pairs[name] = copy

    def up_rows(c):
        return pl.ds(c * LANES, LANES)

    def down_part(c):
        return pl.ds(c * LANES, LANES)

    load("pu", param_up, next_up)
    load("pd", param_down, next_down)
    for c in range(up_chunks):
        load(
            ("up", c),
            slope_up.at[0, pl.ds(mine + c * LANES, LANES), :],
            own_up.at[up_rows(c), :],
        )
    for c in range(down_chunks):
        load(
            ("down", c),
            slope_down.at[0, :, pl.ds(mine + c * LANES, LANES)],
            own_down.at[:, down_part(c)],
        )
    load("sn", slope_norm, own_vec)
    load("pn", param_norm, own_gain)

    barrier = pltpu.get_barrier_semaphore()
    lead = me == replicas - 1

    @pl.when(lead)
    def _():
        pl.semaphore_signal(
            barrier, inc=1, device_id={"replica": other}, device_id_type=MESH
        )

    @pl.when(jnp.logical_not(lead))
    def _():
        pl.semaphore_wait(barrier, 1)
        pl.semaphore_signal(
            pair_ready, inc=1, device_id={"replica": other}, device_id_type=MESH
        )

    @pl.when(lead)
    def _():
        pl.semaphore_wait(pair_ready, 1)
        for k in range(1, models):
            pl.semaphore_signal(
                barrier,
                inc=1,
                device_id={"model": lax.rem(spot + k, models)},
                device_id_type=MESH,
            )

    def meet_models():
        @pl.when(lead)
        def _():
            pl.semaphore_wait(barrier, models - 1)
            pl.semaphore_signal(
                model_ready, inc=1, device_id={"replica": other}, device_id_type=MESH
            )

        @pl.when(jnp.logical_not(lead))
        def _():
            pl.semaphore_wait(model_ready, 1)

    for c in range(up_chunks):
        push(
            ("up", c),
            slope_up.at[0, pl.ds(theirs + c * LANES, LANES), :],
            peer_up.at[up_rows(c), :],
        )
    for c in range(down_chunks):
        push(
            ("down", c),
            slope_down.at[0, :, pl.ds(theirs + c * LANES, LANES)],
            peer_down.at[:, down_part(c)],
        )
    push("sn", slope_norm, peer_vec)
    push("pn", param_norm, peer_gain)

    sent = []

    def share_norm(source, target, sems, i):
        copies = []
        for k in range(1, models):
            copy = pltpu.make_async_remote_copy(
                source.at[i],
                target.at[i, k - 1],
                sems[0].at[i, k - 1],
                sems[1].at[i, k - 1],
                device_id={"model": lax.rem(spot + k, models)},
                device_id_type=MESH,
            )
            copy.start()
            copies.append(copy)
        sent.extend(copies)

        def whole():
            for copy in copies:
                copy.wait_recv()
            total = source[i]
            for k in range(1, models):
                total = total + target[i, k - 1]
            return total

        return whole

    def share_param(i):
        return share_norm(part, got, (norm_send, norm_recv), i)

    def share_slope(i):
        return share_norm(piece, got_piece, (piece_send, piece_recv), i)

    def row_squares(c, value):
        @pl.loop(0, LANES // ROWS)
        def _(r):
            rows = pl.ds(c * LANES + r * ROWS, ROWS)
            total = jnp.zeros((ROWS, LANES), f32)
            for j in range(inner // LANES):
                x = value(rows, pl.ds(j * LANES, LANES))
                total = total + x * x
            square[pl.ds(r * ROWS, ROWS), :] = total

        return jnp.sum(square[...].T, axis=0, keepdims=True)

    def column_squares(c, value):
        def body(r, total):
            for q in range(down_rows // ROWS):
                x = value(pl.ds(r * down_rows + q * ROWS, ROWS), down_part(c))
                total = total + x * x
            return total

        total = lax.fori_loop(
            0, depth // down_rows, body, jnp.zeros((ROWS, LANES), f32)
        )
        return jnp.sum(total, axis=0, keepdims=True)

    def sum_up(rows, lanes):
        return own_up[rows, lanes].astype(f32) + peer_up[rows, lanes].astype(f32)

    def sum_down(rows, lanes):
        return own_down[rows, lanes].astype(f32) + peer_down[rows, lanes].astype(f32)

    loads["pu"].wait()
    for c in range(up_chunks):
        part[0, :, c * LANES : (c + 1) * LANES] = row_squares(
            c, lambda rows, lanes: next_up[rows, lanes]
        )
    meet_models()
    whole_up = share_param(0)

    def measure_down():
        loads["pd"].wait()
        for c in range(down_chunks):
            part[1, :, c * LANES : (c + 1) * LANES] = column_squares(
                c, lambda rows, lanes: next_down[rows, lanes]
            )
        return share_param(1)

    pieces = [("up", c) for c in range(up_chunks)]
    pieces += [("down", c) for c in range(down_chunks)]
    slope_wholes = {}
    param_wholes = {}

    def measure_piece(n):
        kind, c = pieces[n]
        loads[pieces[n]].wait()
        pairs[pieces[n]].wait_recv()
        if kind == "up":
            piece[n] = row_squares(c, lambda rows, lanes: sum_up(rows, lanes) * rate)
        else:
            piece[n] = column_squares(
                c, lambda rows, lanes: sum_down(rows, lanes) * rate
            )
        slope_wholes[n] = share_slope(n)

    def update_piece(n):
        kind, c = pieces[n]
        if kind not in param_wholes:
            total = (whole_up if kind == "up" else whole_down)()
            param_wholes[kind] = jnp.sqrt(total) * (rate * learn_rate)
        ratio = param_wholes[kind][:, c * LANES : (c + 1) * LANES] * lax.rsqrt(
            slope_wholes[n]() + 1e-06
        )
        if kind == "up":
            update_up(c, ratio)
        else:
            update_down(c, ratio)

    def update_up(c, ratio):
        spread[...] = jnp.broadcast_to(ratio, (LANES, LANES)).T

        @pl.loop(0, LANES // ROWS)
        def _(r):
            rows = pl.ds(c * LANES + r * ROWS, ROWS)
            scale = spread[pl.ds(r * ROWS, ROWS), :]
            for j in range(inner // LANES):
                lanes = pl.ds(j * LANES, LANES)
                new = next_up[rows, lanes] - sum_up(rows, lanes) * scale
                next_up[rows, lanes] = new
                half_up[pl.ds(mine + c * LANES + r * ROWS, ROWS), lanes] = new.astype(
                    jnp.bfloat16
                )

        block = half_up.at[pl.ds(mine + c * LANES, LANES), :]
        push(("half_up", c), block, block)

    def update_down(c, ratio):
        scale = jnp.broadcast_to(ratio, (ROWS, LANES))
        lanes = down_part(c)
        place = pl.ds(mine + c * LANES, LANES)

        @pl.loop(0, depth // down_rows)
        def _(r):
            for q in range(down_rows // ROWS):
                rows = pl.ds(r * down_rows + q * ROWS, ROWS)
                new = next_down[rows, lanes] - sum_down(rows, lanes) * scale
                next_down[rows, lanes] = new
                half_down[rows, place] = new.astype(jnp.bfloat16)

        block = half_down.at[:, place]
        push(("half_down", c), block, block)

    ahead = min(AHEAD, len(pieces))
    for n in range(len(pieces) + ahead):
        if n == 2:
            whole_down = measure_down()
        if n < len(pieces):
            measure_piece(n)
        if n >= ahead:
            update_piece(n - ahead)

    loads["sn"].wait()
    loads["pn"].wait()
    pairs["sn"].wait_recv()
    pairs["pn"].wait_recv()
    sum_vec[...] = (
        (own_vec[...].astype(f32) + peer_vec[...].astype(f32)) * rate * learn_rate
    )
    new_gain = own_gain[...].reshape(1, share) - sum_vec[:, pl.ds(mine, share)]
    next_norm[...] = new_gain
    half_norm[:, pl.ds(mine, share)] = new_gain
    half_norm[:, pl.ds(theirs, share)] = (
        peer_gain[...].reshape(1, share) - sum_vec[:, pl.ds(theirs, share)]
    )

    for name, copy in pairs.items():
        copy.wait_send()
        if name[0] in ("half_up", "half_down"):
            copy.wait_recv()
    for copy in sent:
        copy.wait_send()


def write_kernel(
    half_up,
    half_down,
    half_norm,
    next_up,
    next_down,
    next_norm,
    half_up_out,
    half_down_out,
    half_norm_out,
    next_up_out,
    next_down_out,
    next_norm_out,
    sem,
):
    moves = (
        (half_up, half_up_out),
        (half_down, half_down_out),
        (next_up, next_up_out),
        (next_down, next_down_out),
    )
    copies = [
        pltpu.make_async_copy(source, target, sem.at[i])
        for i, (source, target) in enumerate(moves)
    ]
    for copy in copies:
        copy.start()
    half_norm_out[...] = half_norm[...].reshape(half_norm_out.shape).astype(
        jnp.bfloat16
    )
    next_norm_out[...] = next_norm[...].reshape(next_norm_out.shape)
    for copy in copies:
        copy.wait()


def fused(replicas, models, slope_up, slope_down, slope_norm, param_up, param_down, param_norm):
    share, inner = param_up.shape
    depth = param_down.shape[0]
    width = slope_up.shape[1]
    down_chunks = share // LANES
    up_chunks = share // LANES
    moves = up_chunks + down_chunks + 2
    bf16, f32 = jnp.bfloat16, jnp.float32
    hbm = pl.BlockSpec(memory_space=pltpu.HBM)
    vmem = pl.BlockSpec(memory_space=pltpu.VMEM)
    outs = pl.pallas_call(
        functools.partial(update_kernel, replicas, models),
        out_shape=(
            OUT((width, inner), bf16),
            OUT((depth, width), bf16),
            OUT((1, width), f32),
            OUT((share, inner), f32),
            OUT((depth, share), f32),
            OUT((1, share), f32),
        ),
        in_specs=[hbm] * 6,
        out_specs=(vmem,) * 6,
        scratch_shapes=[
            pltpu.VMEM((share, inner), bf16),
            pltpu.VMEM((share, inner), bf16),
            pltpu.VMEM((depth, share), bf16),
            pltpu.VMEM((depth, share), bf16),
            pltpu.VMEM((1, width), bf16),
            pltpu.VMEM((1, width), bf16),
            pltpu.VMEM((share,), f32),
            pltpu.VMEM((share,), f32),
            pltpu.VMEM((1, width), f32),
            pltpu.VMEM((2, 1, share), f32),
            pltpu.VMEM((2, models - 1, 1, share), f32),
            pltpu.VMEM((moves - 2, 1, LANES), f32),
            pltpu.VMEM((moves - 2, models - 1, 1, LANES), f32),
            pltpu.VMEM((LANES, LANES), f32),
            pltpu.VMEM((LANES, LANES), f32),
            pltpu.SemaphoreType.DMA((moves + 2,)),
            pltpu.SemaphoreType.DMA((2 * moves,)),
            pltpu.SemaphoreType.DMA((2 * moves,)),
            pltpu.SemaphoreType.DMA((2, models - 1)),
            pltpu.SemaphoreType.DMA((2, models - 1)),
            pltpu.SemaphoreType.DMA((moves - 2, models - 1)),
            pltpu.SemaphoreType.DMA((moves - 2, models - 1)),
            pltpu.SemaphoreType.REGULAR,
            pltpu.SemaphoreType.REGULAR,
        ],
        compiler_params=pltpu.CompilerParams(
            collective_id=0, has_side_effects=True, vmem_limit_bytes=24 * 2**20
        ),
    )(
        *(
            pltpu.with_memory_space_constraint(x, pltpu.HBM)
            for x in (
                slope_up, slope_down, slope_norm, param_up, param_down, param_norm
            )
        )
    )
    return pl.pallas_call(
        write_kernel,
        out_shape=(
            jax.ShapeDtypeStruct((width, inner), bf16),
            jax.ShapeDtypeStruct((depth, width), bf16),
            jax.ShapeDtypeStruct((width,), bf16),
            jax.ShapeDtypeStruct((share, inner), f32),
            jax.ShapeDtypeStruct((depth, share), f32),
            jax.ShapeDtypeStruct((share,), f32),
        ),
        in_specs=[vmem] * 6,
        out_specs=(hbm, hbm, vmem, hbm, hbm, vmem),
        scratch_shapes=[pltpu.SemaphoreType.DMA((4,))],
        compiler_params=pltpu.CompilerParams(vmem_limit_bytes=24 * 2**20),
    )(*(pltpu.with_memory_space_constraint(x, pltpu.VMEM) for x in outs))


def suits(mesh, *arrays):
    slope_up, param_up, param_down = arrays
    return (
        mesh.shape["replica"] == 2
        and mesh.shape["model"] > 1
        and param_up.shape[0] % LANES == 0
        and param_up.shape[1] % LANES == 0
        and param_down.shape[0] % LANES == 0
    )


def step(mesh, slope_up, slope_down, slope_norm, param_up, param_down, param_norm):
    args = (slope_up, slope_down, slope_norm, param_up, param_down, param_norm)
    if suits(mesh, slope_up, param_up, param_down):
        return fused(mesh.shape["replica"], mesh.shape["model"], *args)
    return shards(*args)


OUT = pltpu.VMEM


def solution(mesh):
    return jax.shard_map(
        functools.partial(step, mesh),
        mesh=mesh,
        in_specs=(
            P(("copy", "replica"), None, "model"),
            P(("copy", "replica"), "model", None),
            P(("copy", "replica"), None),
            P(("copy", "replica"), "model"),
            P(("copy", "model"), "replica"),
            P(("copy", "replica")),
        ),
        out_specs=(
            P("copy", "model"),
            P(("copy", "model"), None),
            P("copy"),
            P(("copy", "replica"), "model"),
            P(("copy", "model"), "replica"),
            P(("copy", "replica")),
        ),
        check_vma=False,
    )
```

```python
import functools

import jax
import jax.numpy as jnp
from jax import lax
from jax.experimental import pallas as pl
from jax.experimental.pallas import tpu as pltpu
from jax.sharding import PartitionSpec as P

learn_rate = 0.5


def shards(slope_up, slope_down, slope_norm, param_up, param_down, param_norm):
    mean_up, mean_down = (
        lax.psum_scatter(
            slope_up[0].astype(jnp.float32).astype(jnp.bfloat16),
            "replica",
            scatter_dimension=0,
            tiled=True,
        ).astype(jnp.float32),
        lax.psum_scatter(
            slope_down[0].astype(jnp.float32).astype(jnp.bfloat16),
            "replica",
            scatter_dimension=1,
            tiled=True,
        ).astype(jnp.float32),
    )
    whole_norm = lax.psum(slope_norm[0].astype(jnp.float32), "replica")
    place = lax.axis_index("replica")
    mean_norm = lax.dynamic_slice_in_dim(
        whole_norm, place * param_norm.shape[0], param_norm.shape[0]
    )
    mean_rate = lax.axis_size("replica") ** (-0.5)
    mean_up = mean_up * mean_rate
    mean_down = mean_down * mean_rate
    mean_norm = mean_norm * mean_rate
    own_up, own_down, slope_up_norm, slope_down_norm = lax.psum(
        (
            jnp.sum(param_up * param_up, axis=1, keepdims=True),
            jnp.sum(param_down * param_down, axis=0, keepdims=True),
            jnp.sum(mean_up * mean_up, axis=1, keepdims=True),
            jnp.sum(mean_down * mean_down, axis=0, keepdims=True),
        ),
        "model",
    )
    mean_up = mean_up * (jnp.sqrt(own_up) * lax.rsqrt(slope_up_norm + 1e-06))
    mean_down = mean_down * (jnp.sqrt(own_down) * lax.rsqrt(slope_down_norm + 1e-06))
    next_up = param_up - learn_rate * mean_up
    next_down = param_down - learn_rate * mean_down
    next_norm = param_norm - learn_rate * mean_norm
    half_up, half_down, half_norm = (
        lax.all_gather(next_up.astype(jnp.bfloat16), "replica", axis=0, tiled=True),
        lax.all_gather(next_down.astype(jnp.bfloat16), "replica", axis=1, tiled=True),
        lax.all_gather(next_norm.astype(jnp.bfloat16), "replica", axis=0, tiled=True),
    )
    return (half_up, half_down, half_norm, next_up, next_down, next_norm)


MESH = pl.DeviceIdType.MESH
LANES = 128
ROWS = 32
AHEAD = 7
DOWN_AT = 5


def update_kernel(
    replicas,
    models,
    slope_up,
    slope_down,
    slope_norm,
    param_up,
    param_down,
    param_norm,
    half_up,
    half_down,
    half_norm,
    next_up,
    next_down,
    next_norm,
    own_up,
    peer_up,
    own_down,
    peer_down,
    own_vec,
    peer_vec,
    own_gain,
    peer_gain,
    sum_vec,
    gain,
    part,
    got,
    piece,
    got_piece,
    square,
    spread,
    load_sem,
    pair_send,
    pair_recv,
    norm_send,
    norm_recv,
    piece_send,
    piece_recv,
    pair_ready,
    model_ready,
):
    me = lax.axis_index("replica")
    other = 1 - me
    spot = lax.axis_index("model")
    share, inner = param_up.shape
    depth = param_down.shape[0]
    up_chunks = share // LANES
    down_chunks = share // LANES
    down_rows = 4 * ROWS
    mine = pl.multiple_of(me * share, LANES)
    theirs = pl.multiple_of(other * share, LANES)
    rate = replicas ** (-0.5)
    f32 = jnp.float32

    loads = {}

    def load(name, source, target):
        copy = pltpu.make_async_copy(source, target, load_sem.at[len(loads)])
        copy.start()
        loads[name] = copy

    pairs = {}

    def push(name, source, target):
        copy = pltpu.make_async_remote_copy(
            source,
            target,
            pair_send.at[len(pairs)],
            pair_recv.at[len(pairs)],
            device_id={"replica": other},
            device_id_type=MESH,
        )
        copy.start()
        pairs[name] = copy

    def up_rows(c):
        return pl.ds(c * LANES, LANES)

    def down_part(c):
        return pl.ds(c * LANES, LANES)

    def load_param_up():
        for c in range(up_chunks):
            load(("pu", c), param_up.at[up_rows(c), :], next_up.at[up_rows(c), :])

    def load_slope_up():
        for c in range(up_chunks):
            load(
                ("up", c),
                slope_up.at[0, pl.ds(mine + c * LANES, LANES), :],
                own_up.at[up_rows(c), :],
            )

    def load_rest():
        for c in range(down_chunks):
            load(
                ("down", c),
                slope_down.at[0, :, pl.ds(mine + c * LANES, LANES)],
                own_down.at[:, down_part(c)],
            )
        load("pd", param_down, next_down)
        load("sn", slope_norm, own_vec)
        load("pn", param_norm, own_gain)

    load_param_up()
    load_slope_up()
    load_rest()

    barrier = pltpu.get_barrier_semaphore()
    lead = me == replicas - 1

    @pl.when(lead)
    def _():
        pl.semaphore_signal(
            barrier, inc=1, device_id={"replica": other}, device_id_type=MESH
        )

    @pl.when(jnp.logical_not(lead))
    def _():
        pl.semaphore_wait(barrier, 1)
        pl.semaphore_signal(
            pair_ready, inc=1, device_id={"replica": other}, device_id_type=MESH
        )

    @pl.when(lead)
    def _():
        pl.semaphore_wait(pair_ready, 1)
        for k in range(1, models):
            pl.semaphore_signal(
                barrier,
                inc=1,
                device_id={"model": lax.rem(spot + k, models)},
                device_id_type=MESH,
            )

    def meet_models():
        @pl.when(lead)
        def _():
            pl.semaphore_wait(barrier, models - 1)
            pl.semaphore_signal(
                model_ready, inc=1, device_id={"replica": other}, device_id_type=MESH
            )

        @pl.when(jnp.logical_not(lead))
        def _():
            pl.semaphore_wait(model_ready, 1)

    for c in range(up_chunks):
        push(
            ("up", c),
            slope_up.at[0, pl.ds(theirs + c * LANES, LANES), :],
            peer_up.at[up_rows(c), :],
        )
    for c in range(down_chunks):
        push(
            ("down", c),
            slope_down.at[0, :, pl.ds(theirs + c * LANES, LANES)],
            peer_down.at[:, down_part(c)],
        )
    push("sn", slope_norm, peer_vec)
    push("pn", param_norm, peer_gain)

    sent = []

    def share_norm(source, target, sems, i):
        copies = []
        for k in range(1, models):
            copy = pltpu.make_async_remote_copy(
                source.at[i],
                target.at[i, k - 1],
                sems[0].at[i, k - 1],
                sems[1].at[i, k - 1],
                device_id={"model": lax.rem(spot + k, models)},
                device_id_type=MESH,
            )
            copy.start()
            copies.append(copy)
        sent.extend(copies)

        def whole():
            for copy in copies:
                copy.wait_recv()
            total = source[i]
            for k in range(1, models):
                total = total + target[i, k - 1]
            return total

        return whole

    def share_param(i):
        return share_norm(part, got, (norm_send, norm_recv), i)

    def share_slope(i):
        return share_norm(piece, got_piece, (piece_send, piece_recv), i)

    def row_squares(c, value):
        @pl.loop(0, LANES // ROWS)
        def _(r):
            rows = pl.ds(c * LANES + r * ROWS, ROWS)
            total = jnp.zeros((ROWS, LANES), f32)
            for j in range(inner // LANES):
                x = value(rows, pl.ds(j * LANES, LANES))
                total = total + x * x
            square[pl.ds(r * ROWS, ROWS), :] = total

        return jnp.sum(square[...].T, axis=0, keepdims=True)

    def column_squares(c, value):
        def body(r, total):
            for q in range(down_rows // ROWS):
                x = value(pl.ds(r * down_rows + q * ROWS, ROWS), down_part(c))
                total = total + x * x
            return total

        total = lax.fori_loop(
            0, depth // down_rows, body, jnp.zeros((ROWS, LANES), f32)
        )
        return jnp.sum(total, axis=0, keepdims=True)

    def sum_up(rows, lanes):
        return own_up[rows, lanes].astype(f32) + peer_up[rows, lanes].astype(f32)

    def sum_down(rows, lanes):
        return own_down[rows, lanes].astype(f32) + peer_down[rows, lanes].astype(f32)

    for c in range(up_chunks):
        loads[("pu", c)].wait()
        part[0, :, c * LANES : (c + 1) * LANES] = row_squares(
            c, lambda rows, lanes: next_up[rows, lanes]
        )
    meet_models()
    whole_up = share_param(0)

    def measure_down():
        loads["pd"].wait()
        for c in range(down_chunks):
            part[1, :, c * LANES : (c + 1) * LANES] = column_squares(
                c, lambda rows, lanes: next_down[rows, lanes]
            )
        return share_param(1)

    pieces = [("up", c) for c in range(up_chunks)]
    pieces += [("down", c) for c in range(down_chunks)]
    slope_wholes = {}
    param_wholes = {}

    def measure_piece(n):
        kind, c = pieces[n]
        loads[pieces[n]].wait()
        pairs[pieces[n]].wait_recv()
        if kind == "up":
            piece[n] = row_squares(c, lambda rows, lanes: sum_up(rows, lanes) * rate)
        else:
            piece[n] = column_squares(
                c, lambda rows, lanes: sum_down(rows, lanes) * rate
            )
        slope_wholes[n] = share_slope(n)

    def update_piece(n):
        kind, c = pieces[n]
        if kind not in param_wholes:
            total = (whole_up if kind == "up" else whole_down)()
            param_wholes[kind] = jnp.sqrt(total) * (rate * learn_rate)
        ratio = param_wholes[kind][:, c * LANES : (c + 1) * LANES] * lax.rsqrt(
            slope_wholes[n]() + 1e-06
        )
        if kind == "up":
            update_up(c, ratio)
        else:
            update_down(c, ratio)

    def update_up(c, ratio):
        spread[...] = jnp.broadcast_to(ratio, (LANES, LANES)).T

        @pl.loop(0, LANES // ROWS)
        def _(r):
            rows = pl.ds(c * LANES + r * ROWS, ROWS)
            scale = spread[pl.ds(r * ROWS, ROWS), :]
            for j in range(inner // LANES):
                lanes = pl.ds(j * LANES, LANES)
                new = next_up[rows, lanes] - sum_up(rows, lanes) * scale
                next_up[rows, lanes] = new
                half_up[pl.ds(mine + c * LANES + r * ROWS, ROWS), lanes] = new.astype(
                    jnp.bfloat16
                )

        block = half_up.at[pl.ds(mine + c * LANES, LANES), :]
        push(("half_up", c), block, block)

    def update_down(c, ratio):
        scale = jnp.broadcast_to(ratio, (ROWS, LANES))
        lanes = down_part(c)
        place = pl.ds(mine + c * LANES, LANES)

        @pl.loop(0, depth // down_rows)
        def _(r):
            for q in range(down_rows // ROWS):
                rows = pl.ds(r * down_rows + q * ROWS, ROWS)
                new = next_down[rows, lanes] - sum_down(rows, lanes) * scale
                next_down[rows, lanes] = new
                half_down[rows, place] = new.astype(jnp.bfloat16)

        block = half_down.at[:, place]
        push(("half_down", c), block, block)

    def update_norm():
        loads["sn"].wait()
        loads["pn"].wait()
        pairs["sn"].wait_recv()
        pairs["pn"].wait_recv()
        sum_vec[...] = (
            (own_vec[...].astype(f32) + peer_vec[...].astype(f32)) * rate * learn_rate
        )
        new_gain = own_gain[...].reshape(1, share) - sum_vec[:, pl.ds(mine, share)]
        gain[:, pl.ds(mine, share)] = new_gain
        gain[:, pl.ds(theirs, share)] = (
            peer_gain[...].reshape(1, share) - sum_vec[:, pl.ds(theirs, share)]
        )
        next_norm[...] = new_gain.reshape(share)
        half_norm[...] = gain[...].reshape(half_norm.shape).astype(jnp.bfloat16)

    ahead = min(AHEAD, len(pieces))
    for n in range(len(pieces) + ahead):
        if n == min(DOWN_AT, up_chunks):
            whole_down = measure_down()
        if n < len(pieces):
            measure_piece(n)
        if n >= ahead:
            update_piece(n - ahead)
    update_norm()


    for name, copy in pairs.items():
        copy.wait_send()
        if name[0] in ("half_up", "half_down"):
            copy.wait_recv()
    for copy in sent:
        copy.wait_send()


def write_kernel(
    half_up,
    half_down,
    half_norm,
    next_up,
    next_down,
    next_norm,
    half_up_out,
    half_down_out,
    half_norm_out,
    next_up_out,
    next_down_out,
    next_norm_out,
    sem,
):
    moves = (
        (half_norm, half_norm_out),
        (next_norm, next_norm_out),
        (half_up, half_up_out),
        (half_down, half_down_out),
        (next_up, next_up_out),
        (next_down, next_down_out),
    )
    copies = []
    for source, target in moves:
        cuts = 2 if len(source.shape) == 2 else 1
        rows = source.shape[0] // cuts
        for i in range(cuts):
            part = pl.ds(i * rows, rows)
            copies.append(
                pltpu.make_async_copy(
                    source.at[part], target.at[part], sem.at[len(copies)]
                )
            )
    for copy in copies:
        copy.start()
    for copy in copies:
        copy.wait()


def fused(replicas, models, slope_up, slope_down, slope_norm, param_up, param_down, param_norm):
    share, inner = param_up.shape
    depth = param_down.shape[0]
    width = slope_up.shape[1]
    down_chunks = share // LANES
    up_chunks = share // LANES
    moves = up_chunks + down_chunks + 2
    bf16, f32 = jnp.bfloat16, jnp.float32
    hbm = pl.BlockSpec(memory_space=pltpu.HBM)
    vmem = pl.BlockSpec(memory_space=pltpu.VMEM)
    outs = pl.pallas_call(
        functools.partial(update_kernel, replicas, models),
        out_shape=(
            OUT((width, inner), bf16),
            OUT((depth, width), bf16),
            OUT((width,), bf16),
            OUT((share, inner), f32),
            OUT((depth, share), f32),
            OUT((share,), f32),
        ),
        in_specs=[hbm] * 6,
        out_specs=(vmem,) * 6,
        scratch_shapes=[
            pltpu.VMEM((share, inner), bf16),
            pltpu.VMEM((share, inner), bf16),
            pltpu.VMEM((depth, share), bf16),
            pltpu.VMEM((depth, share), bf16),
            pltpu.VMEM((1, width), bf16),
            pltpu.VMEM((1, width), bf16),
            pltpu.VMEM((share,), f32),
            pltpu.VMEM((share,), f32),
            pltpu.VMEM((1, width), f32),
            pltpu.VMEM((1, width), f32),
            pltpu.VMEM((2, 1, share), f32),
            pltpu.VMEM((2, models - 1, 1, share), f32),
            pltpu.VMEM((moves - 2, 1, LANES), f32),
            pltpu.VMEM((moves - 2, models - 1, 1, LANES), f32),
            pltpu.VMEM((LANES, LANES), f32),
            pltpu.VMEM((LANES, LANES), f32),
            pltpu.SemaphoreType.DMA((moves + up_chunks + 1,)),
            pltpu.SemaphoreType.DMA((2 * moves,)),
            pltpu.SemaphoreType.DMA((2 * moves,)),
            pltpu.SemaphoreType.DMA((2, models - 1)),
            pltpu.SemaphoreType.DMA((2, models - 1)),
            pltpu.SemaphoreType.DMA((moves - 2, models - 1)),
            pltpu.SemaphoreType.DMA((moves - 2, models - 1)),
            pltpu.SemaphoreType.REGULAR,
            pltpu.SemaphoreType.REGULAR,
        ],
        compiler_params=pltpu.CompilerParams(
            collective_id=0, has_side_effects=True, vmem_limit_bytes=24 * 2**20
        ),
    )(
        *(
            pltpu.with_memory_space_constraint(x, pltpu.HBM)
            for x in (
                slope_up, slope_down, slope_norm, param_up, param_down, param_norm
            )
        )
    )
    return pl.pallas_call(
        write_kernel,
        out_shape=(
            jax.ShapeDtypeStruct((width, inner), bf16),
            jax.ShapeDtypeStruct((depth, width), bf16),
            jax.ShapeDtypeStruct((width,), bf16),
            jax.ShapeDtypeStruct((share, inner), f32),
            jax.ShapeDtypeStruct((depth, share), f32),
            jax.ShapeDtypeStruct((share,), f32),
        ),
        in_specs=[vmem] * 6,
        out_specs=(hbm,) * 6,
        scratch_shapes=[pltpu.SemaphoreType.DMA((10,))],
        compiler_params=pltpu.CompilerParams(vmem_limit_bytes=24 * 2**20),
    )(*(pltpu.with_memory_space_constraint(x, pltpu.VMEM) for x in outs))


def suits(mesh, *arrays):
    slope_up, param_up, param_down = arrays
    return (
        mesh.shape["replica"] == 2
        and mesh.shape["model"] > 1
        and param_up.shape[0] % LANES == 0
        and param_up.shape[1] % LANES == 0
        and param_down.shape[0] % LANES == 0
    )


def step(mesh, slope_up, slope_down, slope_norm, param_up, param_down, param_norm):
    args = (slope_up, slope_down, slope_norm, param_up, param_down, param_norm)
    if suits(mesh, slope_up, param_up, param_down):
        return fused(mesh.shape["replica"], mesh.shape["model"], *args)
    return shards(*args)


OUT = pltpu.VMEM


def solution(mesh):
    return jax.shard_map(
        functools.partial(step, mesh),
        mesh=mesh,
        in_specs=(
            P(("copy", "replica"), None, "model"),
            P(("copy", "replica"), "model", None),
            P(("copy", "replica"), None),
            P(("copy", "replica"), "model"),
            P(("copy", "model"), "replica"),
            P(("copy", "replica")),
        ),
        out_specs=(
            P("copy", "model"),
            P(("copy", "model"), None),
            P("copy"),
            P(("copy", "replica"), "model"),
            P(("copy", "model"), "replica"),
            P(("copy", "replica")),
        ),
        check_vma=False,
    )
```

```python
import functools

import jax
import jax.numpy as jnp
from jax import lax
from jax.experimental import pallas as pl
from jax.experimental.pallas import tpu as pltpu
from jax.sharding import PartitionSpec as P

learn_rate = 0.5


def shards(slope_up, slope_down, slope_norm, param_up, param_down, param_norm):
    mean_up, mean_down = (
        lax.psum_scatter(
            slope_up[0].astype(jnp.float32).astype(jnp.bfloat16),
            "replica",
            scatter_dimension=0,
            tiled=True,
        ).astype(jnp.float32),
        lax.psum_scatter(
            slope_down[0].astype(jnp.float32).astype(jnp.bfloat16),
            "replica",
            scatter_dimension=1,
            tiled=True,
        ).astype(jnp.float32),
    )
    whole_norm = lax.psum(slope_norm[0].astype(jnp.float32), "replica")
    place = lax.axis_index("replica")
    mean_norm = lax.dynamic_slice_in_dim(
        whole_norm, place * param_norm.shape[0], param_norm.shape[0]
    )
    mean_rate = lax.axis_size("replica") ** (-0.5)
    mean_up = mean_up * mean_rate
    mean_down = mean_down * mean_rate
    mean_norm = mean_norm * mean_rate
    own_up, own_down, slope_up_norm, slope_down_norm = lax.psum(
        (
            jnp.sum(param_up * param_up, axis=1, keepdims=True),
            jnp.sum(param_down * param_down, axis=0, keepdims=True),
            jnp.sum(mean_up * mean_up, axis=1, keepdims=True),
            jnp.sum(mean_down * mean_down, axis=0, keepdims=True),
        ),
        "model",
    )
    mean_up = mean_up * (jnp.sqrt(own_up) * lax.rsqrt(slope_up_norm + 1e-06))
    mean_down = mean_down * (jnp.sqrt(own_down) * lax.rsqrt(slope_down_norm + 1e-06))
    next_up = param_up - learn_rate * mean_up
    next_down = param_down - learn_rate * mean_down
    next_norm = param_norm - learn_rate * mean_norm
    half_up, half_down, half_norm = (
        lax.all_gather(next_up.astype(jnp.bfloat16), "replica", axis=0, tiled=True),
        lax.all_gather(next_down.astype(jnp.bfloat16), "replica", axis=1, tiled=True),
        lax.all_gather(next_norm.astype(jnp.bfloat16), "replica", axis=0, tiled=True),
    )
    return (half_up, half_down, half_norm, next_up, next_down, next_norm)


MESH = pl.DeviceIdType.MESH
LANES = 128
ROWS = 32
AHEAD = 9


def update_kernel(
    replicas,
    models,
    slope_up,
    slope_down,
    slope_norm,
    param_up,
    param_down,
    param_norm,
    half_up,
    half_down,
    half_norm,
    next_up,
    next_down,
    next_norm,
    own_up,
    peer_up,
    own_down,
    peer_down,
    own_vec,
    peer_vec,
    own_gain,
    peer_gain,
    sum_vec,
    gain,
    piece,
    got_piece,
    square,
    spread,
    load_sem,
    send_sem,
    slope_recv,
    half_recv,
    piece_recv,
    pair_ready,
    model_ready,
):
    me = lax.axis_index("replica")
    other = 1 - me
    spot = lax.axis_index("model")
    share, inner = param_up.shape
    depth = param_down.shape[0]
    down_rows = 4 * ROWS
    mine = pl.multiple_of(me * share, LANES)
    theirs = pl.multiple_of(other * share, LANES)
    rate = replicas ** (-0.5)
    f32 = jnp.float32
    pieces = pieces_of(share)

    loads = {}

    def load(name, source, target):
        copy = pltpu.make_async_copy(source, target, load_sem.at[len(loads)])
        copy.start()
        loads[name] = copy

    def pair_copy(source, target, send, recv):
        return pltpu.make_async_remote_copy(
            source,
            target,
            send_sem.at[send],
            recv,
            device_id={"replica": other},
            device_id_type=MESH,
        )

    def own_slope(kind, start, size):
        if kind == "up":
            return slope_up.at[0, pl.ds(mine + start, size), :]
        return slope_down.at[0, :, pl.ds(mine + start, size)]

    def peer_slope(kind, start, size):
        if kind == "up":
            return slope_up.at[0, pl.ds(theirs + start, size), :]
        return slope_down.at[0, :, pl.ds(theirs + start, size)]

    def half(kind, start, size):
        if kind == "up":
            return half_up.at[pl.ds(start, size), :]
        return half_down.at[:, pl.ds(start, size)]

    def cut(kind, up, down, start, size):
        if kind == "up":
            return up.at[pl.ds(start, size), :]
        return down.at[:, pl.ds(start, size)]

    first = {}
    parts = [("down", 0, LANES), ("down", LANES, share - LANES), ("up", 0, share)]
    for span in parts:
        if span[2]:
            load(
                ("param", span),
                cut(span[0], param_up, param_down, *span[1:]),
                cut(span[0], next_up, next_down, *span[1:]),
            )
            load(
                ("slope", span),
                own_slope(*span),
                cut(span[0], own_up, own_down, *span[1:]),
            )
            for piece_span in pieces:
                if piece_span[0] == span[0] and piece_span[1] == span[1]:
                    first[piece_span] = span
    load("slope norm", slope_norm, own_vec)
    load("param norm", param_norm, own_gain)

    barrier = pltpu.get_barrier_semaphore()
    lead = me == replicas - 1

    @pl.when(lead)
    def _():
        pl.semaphore_signal(
            barrier, inc=1, device_id={"replica": other}, device_id_type=MESH
        )

    @pl.when(jnp.logical_not(lead))
    def _():
        pl.semaphore_wait(barrier, 1)
        pl.semaphore_signal(
            pair_ready, inc=1, device_id={"replica": other}, device_id_type=MESH
        )

    @pl.when(lead)
    def _():
        pl.semaphore_wait(pair_ready, 1)
        for k in range(1, models):
            pl.semaphore_signal(
                barrier,
                inc=1,
                device_id={"model": lax.rem(spot + k, models)},
                device_id_type=MESH,
            )

    def meet_models():
        @pl.when(lead)
        def _():
            pl.semaphore_wait(barrier, models - 1)
            pl.semaphore_signal(
                model_ready, inc=1, device_id={"replica": other}, device_id_type=MESH
            )

        @pl.when(jnp.logical_not(lead))
        def _():
            pl.semaphore_wait(model_ready, 1)

    for n, span in enumerate(pieces):
        pair_copy(
            peer_slope(*span),
            cut(span[0], peer_up, peer_down, *span[1:]),
            0 if span[0] == "up" else 1,
            slope_recv.at[n],
        ).start()
    norms = [
        pair_copy(slope_norm, peer_vec, 2, slope_recv.at[len(pieces)]),
        pair_copy(param_norm, peer_gain, 3, slope_recv.at[len(pieces) + 1]),
    ]
    for copy in norms:
        copy.start()

    def norm_copy(source, target, n, k):
        return pltpu.make_async_remote_copy(
            source,
            target,
            send_sem.at[6],
            piece_recv.at[n],
            device_id={"model": lax.rem(spot + k, models)},
            device_id_type=MESH,
        )

    def share_norm(n):
        for k in range(1, models):
            norm_copy(piece.at[n], got_piece.at[n, k - 1], n, k).start()

    def whole_norm(n):
        norm_copy(got_piece.at[n], got_piece.at[n], n, 1).wait_recv()
        total = piece[n]
        for k in range(1, models):
            total = total + got_piece[n, k - 1]
        return total

    square[...] = jnp.zeros(square.shape, f32)

    def row_squares(start, size, value):
        @pl.loop(0, size // ROWS)
        def _(r):
            rows = pl.ds(start + r * ROWS, ROWS)
            total = jnp.zeros((ROWS, LANES), f32)
            for j in range(inner // LANES):
                x = value(rows, pl.ds(j * LANES, LANES))
                total = total + x * x
            square[pl.ds(r * ROWS, ROWS), :] = total

        return jnp.sum(square[...].T, axis=0, keepdims=True)

    def column_squares(start, size, value):
        def body(r, total):
            for q in range(down_rows // ROWS):
                x = value(pl.ds(r * down_rows + q * ROWS, ROWS), pl.ds(start, size))
                total = total + x * x
            return total

        total = lax.fori_loop(
            0, depth // down_rows, body, jnp.zeros((ROWS, LANES), f32)
        )
        return jnp.sum(total, axis=0, keepdims=True)

    def sum_up(rows, lanes):
        return own_up[rows, lanes].astype(f32) + peer_up[rows, lanes].astype(f32)

    def sum_down(rows, lanes):
        return own_down[rows, lanes].astype(f32) + peer_down[rows, lanes].astype(f32)

    def measure_piece(n):
        kind, start, size = pieces[n]
        squares = row_squares if kind == "up" else column_squares
        param = next_up if kind == "up" else next_down
        total = sum_up if kind == "up" else sum_down
        span = first.get(pieces[n])
        if span:
            loads["param", span].wait()
        piece[n, 0:1] = squares(start, size, lambda rows, lanes: param[rows, lanes])
        if span:
            loads["slope", span].wait()
        pair_copy(
            peer_slope(*pieces[n]),
            cut(kind, peer_up, peer_down, start, size),
            0,
            slope_recv.at[n],
        ).wait_recv()
        piece[n, 1:2] = squares(
            start, size, lambda rows, lanes: total(rows, lanes) * rate
        )
        if n == 0:
            meet_models()
        share_norm(n)

    def update_piece(n):
        kind, start, size = pieces[n]
        whole = whole_norm(n)
        ratio = jnp.sqrt(whole[0:1]) * (rate * learn_rate) * lax.rsqrt(
            whole[1:2] + 1e-06
        )
        if kind == "up":
            update_up(start, size, ratio)
        else:
            update_down(start, size, ratio)
        block = half(kind, mine + start, size)
        which = 0 if kind == "up" else 1
        pair_copy(block, block, 4 + which, half_recv.at[which]).start()

    def update_up(start, size, ratio):
        spread[...] = jnp.broadcast_to(ratio, (LANES, LANES)).T

        @pl.loop(0, size // ROWS)
        def _(r):
            rows = pl.ds(start + r * ROWS, ROWS)
            scale = spread[pl.ds(r * ROWS, ROWS), :]
            for j in range(inner // LANES):
                lanes = pl.ds(j * LANES, LANES)
                new = next_up[rows, lanes] - sum_up(rows, lanes) * scale
                next_up[rows, lanes] = new
                half_up[pl.ds(mine + start + r * ROWS, ROWS), lanes] = new.astype(
                    jnp.bfloat16
                )

    def update_down(start, size, ratio):
        scale = jnp.broadcast_to(ratio, (ROWS, LANES))
        lanes = pl.ds(start, size)
        place = pl.ds(mine + start, size)

        @pl.loop(0, depth // down_rows)
        def _(r):
            for q in range(down_rows // ROWS):
                rows = pl.ds(r * down_rows + q * ROWS, ROWS)
                new = next_down[rows, lanes] - sum_down(rows, lanes) * scale
                next_down[rows, lanes] = new
                half_down[rows, place] = new.astype(jnp.bfloat16)

    def update_norm():
        loads["slope norm"].wait()
        loads["param norm"].wait()
        for copy in norms:
            copy.wait_recv()
        sum_vec[...] = (
            (own_vec[...].astype(f32) + peer_vec[...].astype(f32)) * rate * learn_rate
        )
        new_gain = own_gain[...].reshape(1, share) - sum_vec[:, pl.ds(mine, share)]
        gain[:, pl.ds(mine, share)] = new_gain
        gain[:, pl.ds(theirs, share)] = (
            peer_gain[...].reshape(1, share) - sum_vec[:, pl.ds(theirs, share)]
        )
        next_norm[...] = new_gain.reshape(share)
        half_norm[...] = gain[...].reshape(half_norm.shape).astype(jnp.bfloat16)

    ahead = min(AHEAD, len(pieces))
    for n in range(len(pieces) + ahead):
        if n < len(pieces):
            measure_piece(n)
        if n >= ahead:
            update_piece(n - ahead)
    update_norm()

    for which, kind in enumerate(("up", "down")):
        pair_copy(
            peer_slope(kind, 0, share),
            cut(kind, peer_up, peer_down, 0, share),
            which,
            half_recv.at[which],
        ).wait_send()
        halves = pair_copy(
            half(kind, mine, share),
            half(kind, theirs, share),
            4 + which,
            half_recv.at[which],
        )
        halves.wait_send()
        halves.wait_recv()
    for copy in norms:
        copy.wait_send()
    norm_copy(got_piece, got_piece, 0, 1).wait_send()


def pieces_of(share):
    pieces = [("down", start, LANES) for start in range(0, share, LANES)]
    pieces += [("up", start, LANES) for start in range(0, share, LANES)]
    return pieces


def write_kernel(
    half_up,
    half_down,
    half_norm,
    next_up,
    next_down,
    next_norm,
    half_up_out,
    half_down_out,
    half_norm_out,
    next_up_out,
    next_down_out,
    next_norm_out,
    sem,
):
    moves = (
        (half_norm, half_norm_out),
        (next_norm, next_norm_out),
        (half_up, half_up_out),
        (half_down, half_down_out),
        (next_up, next_up_out),
        (next_down, next_down_out),
    )
    copies = []
    for source, target in moves:
        cuts = 2 if len(source.shape) == 2 else 1
        rows = source.shape[0] // cuts
        for i in range(cuts):
            part = pl.ds(i * rows, rows)
            copies.append(
                pltpu.make_async_copy(
                    source.at[part], target.at[part], sem.at[len(copies)]
                )
            )
    for copy in copies:
        copy.start()
    for copy in copies:
        copy.wait()


def fused(replicas, models, slope_up, slope_down, slope_norm, param_up, param_down, param_norm):
    share, inner = param_up.shape
    depth = param_down.shape[0]
    width = slope_up.shape[1]
    count = len(pieces_of(share))
    bf16, f32 = jnp.bfloat16, jnp.float32
    hbm = pl.BlockSpec(memory_space=pltpu.HBM)
    vmem = pl.BlockSpec(memory_space=pltpu.VMEM)
    outs = pl.pallas_call(
        functools.partial(update_kernel, replicas, models),
        out_shape=(
            OUT((width, inner), bf16),
            OUT((depth, width), bf16),
            OUT((width,), bf16),
            OUT((share, inner), f32),
            OUT((depth, share), f32),
            OUT((share,), f32),
        ),
        in_specs=[hbm] * 6,
        out_specs=(vmem,) * 6,
        scratch_shapes=[
            pltpu.VMEM((share, inner), bf16),
            pltpu.VMEM((share, inner), bf16),
            pltpu.VMEM((depth, share), bf16),
            pltpu.VMEM((depth, share), bf16),
            pltpu.VMEM((1, width), bf16),
            pltpu.VMEM((1, width), bf16),
            pltpu.VMEM((share,), f32),
            pltpu.VMEM((share,), f32),
            pltpu.VMEM((1, width), f32),
            pltpu.VMEM((1, width), f32),
            pltpu.VMEM((count, 2, LANES), f32),
            pltpu.VMEM((count, models - 1, 2, LANES), f32),
            pltpu.VMEM((LANES, LANES), f32),
            pltpu.VMEM((LANES, LANES), f32),
            pltpu.SemaphoreType.DMA((8,)),
            pltpu.SemaphoreType.DMA((7,)),
            pltpu.SemaphoreType.DMA((count + 2,)),
            pltpu.SemaphoreType.DMA((2,)),
            pltpu.SemaphoreType.DMA((count,)),
            pltpu.SemaphoreType.REGULAR,
            pltpu.SemaphoreType.REGULAR,
        ],
        compiler_params=pltpu.CompilerParams(
            collective_id=0, has_side_effects=True, vmem_limit_bytes=24 * 2**20
        ),
    )(
        *(
            pltpu.with_memory_space_constraint(x, pltpu.HBM)
            for x in (
                slope_up, slope_down, slope_norm, param_up, param_down, param_norm
            )
        )
    )
    return pl.pallas_call(
        write_kernel,
        out_shape=(
            jax.ShapeDtypeStruct((width, inner), bf16),
            jax.ShapeDtypeStruct((depth, width), bf16),
            jax.ShapeDtypeStruct((width,), bf16),
            jax.ShapeDtypeStruct((share, inner), f32),
            jax.ShapeDtypeStruct((depth, share), f32),
            jax.ShapeDtypeStruct((share,), f32),
        ),
        in_specs=[vmem] * 6,
        out_specs=(hbm,) * 6,
        scratch_shapes=[pltpu.SemaphoreType.DMA((10,))],
        compiler_params=pltpu.CompilerParams(vmem_limit_bytes=24 * 2**20),
    )(*(pltpu.with_memory_space_constraint(x, pltpu.VMEM) for x in outs))


def suits(mesh, *arrays):
    slope_up, param_up, param_down = arrays
    return (
        mesh.shape["replica"] == 2
        and mesh.shape["model"] > 1
        and param_up.shape[0] % LANES == 0
        and param_up.shape[1] % LANES == 0
        and param_down.shape[0] % LANES == 0
    )


def step(mesh, slope_up, slope_down, slope_norm, param_up, param_down, param_norm):
    args = (slope_up, slope_down, slope_norm, param_up, param_down, param_norm)
    if suits(mesh, slope_up, param_up, param_down):
        return fused(mesh.shape["replica"], mesh.shape["model"], *args)
    return shards(*args)


OUT = pltpu.VMEM


def solution(mesh):
    return jax.shard_map(
        functools.partial(step, mesh),
        mesh=mesh,
        in_specs=(
            P(("copy", "replica"), None, "model"),
            P(("copy", "replica"), "model", None),
            P(("copy", "replica"), None),
            P(("copy", "replica"), "model"),
            P(("copy", "model"), "replica"),
            P(("copy", "replica")),
        ),
        out_specs=(
            P("copy", "model"),
            P(("copy", "model"), None),
            P("copy"),
            P(("copy", "replica"), "model"),
            P(("copy", "model"), "replica"),
            P(("copy", "replica")),
        ),
        check_vma=False,
    )
```

```python
import functools

import jax
import jax.numpy as jnp
from jax import lax
from jax.experimental import pallas as pl
from jax.experimental.pallas import tpu as pltpu
from jax.sharding import PartitionSpec as P

learn_rate = 0.5


def shards(slope_up, slope_down, slope_norm, param_up, param_down, param_norm):
    mean_up, mean_down = (
        lax.psum_scatter(
            slope_up[0].astype(jnp.float32).astype(jnp.bfloat16),
            "replica",
            scatter_dimension=0,
            tiled=True,
        ).astype(jnp.float32),
        lax.psum_scatter(
            slope_down[0].astype(jnp.float32).astype(jnp.bfloat16),
            "replica",
            scatter_dimension=1,
            tiled=True,
        ).astype(jnp.float32),
    )
    whole_norm = lax.psum(slope_norm[0].astype(jnp.float32), "replica")
    place = lax.axis_index("replica")
    mean_norm = lax.dynamic_slice_in_dim(
        whole_norm, place * param_norm.shape[0], param_norm.shape[0]
    )
    mean_rate = lax.axis_size("replica") ** (-0.5)
    mean_up = mean_up * mean_rate
    mean_down = mean_down * mean_rate
    mean_norm = mean_norm * mean_rate
    own_up, own_down, slope_up_norm, slope_down_norm = lax.psum(
        (
            jnp.sum(param_up * param_up, axis=1, keepdims=True),
            jnp.sum(param_down * param_down, axis=0, keepdims=True),
            jnp.sum(mean_up * mean_up, axis=1, keepdims=True),
            jnp.sum(mean_down * mean_down, axis=0, keepdims=True),
        ),
        "model",
    )
    mean_up = mean_up * (jnp.sqrt(own_up) * lax.rsqrt(slope_up_norm + 1e-06))
    mean_down = mean_down * (jnp.sqrt(own_down) * lax.rsqrt(slope_down_norm + 1e-06))
    next_up = param_up - learn_rate * mean_up
    next_down = param_down - learn_rate * mean_down
    next_norm = param_norm - learn_rate * mean_norm
    half_up, half_down, half_norm = (
        lax.all_gather(next_up.astype(jnp.bfloat16), "replica", axis=0, tiled=True),
        lax.all_gather(next_down.astype(jnp.bfloat16), "replica", axis=1, tiled=True),
        lax.all_gather(next_norm.astype(jnp.bfloat16), "replica", axis=0, tiled=True),
    )
    return (half_up, half_down, half_norm, next_up, next_down, next_norm)


MESH = pl.DeviceIdType.MESH
LANES = 128
ROWS = 32
AHEAD = 8
UP_CUTS = 2
DOWN_CUTS = 2


def update_kernel(
    replicas,
    models,
    slope_up,
    slope_down,
    slope_norm,
    param_up,
    param_down,
    param_norm,
    half_up,
    half_down,
    half_norm,
    next_up,
    next_down,
    next_norm,
    own_up,
    peer_up,
    own_down,
    peer_down,
    own_vec,
    peer_vec,
    own_gain,
    peer_gain,
    sum_vec,
    gain,
    piece,
    got_piece,
    square,
    spread,
    load_sem,
    send_sem,
    slope_recv,
    half_recv,
    piece_recv,
    pair_ready,
    model_ready,
):
    me = lax.axis_index("replica")
    other = 1 - me
    spot = lax.axis_index("model")
    share, inner = param_up.shape
    depth = param_down.shape[0]
    down_rows = 10 * ROWS
    mine = pl.multiple_of(me * share, LANES)
    theirs = pl.multiple_of(other * share, LANES)
    rate = replicas ** (-0.5)
    f32 = jnp.float32
    pieces = pieces_of(share)

    loads = {}

    def load(name, source, target):
        copy = pltpu.make_async_copy(source, target, load_sem.at[len(loads)])
        copy.start()
        loads[name] = copy

    def pair_copy(source, target, send, recv):
        return pltpu.make_async_remote_copy(
            source,
            target,
            send_sem.at[send],
            recv,
            device_id={"replica": other},
            device_id_type=MESH,
        )

    def own_slope(kind, start, size):
        if kind == "up":
            return slope_up.at[0, pl.ds(mine + start, size), :]
        return slope_down.at[0, :, pl.ds(mine + start, size)]

    def peer_slope(kind, start, size):
        if kind == "up":
            return slope_up.at[0, pl.ds(theirs + start, size), :]
        return slope_down.at[0, :, pl.ds(theirs + start, size)]

    def half(kind, start, size):
        if kind == "up":
            return half_up.at[pl.ds(start, size), :]
        return half_down.at[:, pl.ds(start, size)]

    def cut(kind, up, down, start, size):
        if kind == "up":
            return up.at[pl.ds(start, size), :]
        return down.at[:, pl.ds(start, size)]

    barrier = pltpu.get_barrier_semaphore()
    lead = me == replicas - 1

    @pl.when(lead)
    def _():
        pl.semaphore_signal(
            barrier, inc=1, device_id={"replica": other}, device_id_type=MESH
        )

    @pl.when(jnp.logical_not(lead))
    def _():
        pl.semaphore_wait(barrier, 1)
        pl.semaphore_signal(
            pair_ready, inc=1, device_id={"replica": other}, device_id_type=MESH
        )

    first = {}
    parts = [("down", 0, LANES), ("down", LANES, share - LANES), ("up", 0, share)]
    for span in parts:
        if span[2]:
            load(
                ("param", span),
                cut(span[0], param_up, param_down, *span[1:]),
                cut(span[0], next_up, next_down, *span[1:]),
            )
            load(
                ("slope", span),
                own_slope(*span),
                cut(span[0], own_up, own_down, *span[1:]),
            )
            for piece_span in pieces:
                if piece_span[0] == span[0] and piece_span[1] == span[1]:
                    first[piece_span] = span
    load("slope norm", slope_norm, own_vec)
    load("param norm", param_norm, own_gain)

    @pl.when(lead)
    def _():
        pl.semaphore_wait(pair_ready, 1)
        for k in range(1, models):
            pl.semaphore_signal(
                barrier,
                inc=1,
                device_id={"model": lax.rem(spot + k, models)},
                device_id_type=MESH,
            )

    def meet_models():
        @pl.when(lead)
        def _():
            pl.semaphore_wait(barrier, models - 1)
            pl.semaphore_signal(
                model_ready, inc=1, device_id={"replica": other}, device_id_type=MESH
            )

        @pl.when(jnp.logical_not(lead))
        def _():
            pl.semaphore_wait(model_ready, 1)

    for n, span in enumerate(pieces):
        pair_copy(
            peer_slope(*span),
            cut(span[0], peer_up, peer_down, *span[1:]),
            0 if span[0] == "up" else 1,
            slope_recv.at[n],
        ).start()
    norms = [
        pair_copy(slope_norm, peer_vec, 2, slope_recv.at[len(pieces)]),
        pair_copy(param_norm, peer_gain, 3, slope_recv.at[len(pieces) + 1]),
    ]
    for copy in norms:
        copy.start()

    def norm_copy(source, target, n, k):
        return pltpu.make_async_remote_copy(
            source,
            target,
            send_sem.at[6],
            piece_recv.at[n],
            device_id={"model": lax.rem(spot + k, models)},
            device_id_type=MESH,
        )

    def share_norm(n):
        for k in range(1, models):
            norm_copy(piece.at[n], got_piece.at[n, k - 1], n, k).start()

    def whole_norm(n):
        norm_copy(got_piece.at[n], got_piece.at[n], n, 1).wait_recv()
        total = piece[n]
        for k in range(1, models):
            total = total + got_piece[n, k - 1]
        return total

    square[...] = jnp.zeros(square.shape, f32)

    def row_squares(start, size, value):
        for r in range(size // ROWS):
            rows = pl.ds(start + r * ROWS, ROWS)
            total = jnp.zeros((ROWS, LANES), f32)
            for j in range(inner // LANES):
                x = value(rows, pl.ds(j * LANES, LANES))
                total = total + x * x
            square[pl.ds(r * ROWS, ROWS), :] = total

        return jnp.sum(square[...].T, axis=0, keepdims=True)

    def column_squares(start, size, value):
        def body(r, total):
            for q in range(down_rows // ROWS):
                x = value(pl.ds(r * down_rows + q * ROWS, ROWS), pl.ds(start, size))
                total = total + x * x
            return total

        total = lax.fori_loop(
            0, depth // down_rows, body, jnp.zeros((ROWS, LANES), f32)
        )
        return jnp.sum(total, axis=0, keepdims=True)

    def sum_up(rows, lanes):
        return own_up[rows, lanes].astype(f32) + peer_up[rows, lanes].astype(f32)

    def sum_down(rows, lanes):
        return own_down[rows, lanes].astype(f32) + peer_down[rows, lanes].astype(f32)

    def measure_piece(n):
        kind, start, size = pieces[n]
        squares = row_squares if kind == "up" else column_squares
        param = next_up if kind == "up" else next_down
        total = sum_up if kind == "up" else sum_down
        span = first.get(pieces[n])
        if span:
            loads["param", span].wait()
        piece[n, 0:1] = squares(start, size, lambda rows, lanes: param[rows, lanes])
        if span:
            loads["slope", span].wait()
        pair_copy(
            peer_slope(*pieces[n]),
            cut(kind, peer_up, peer_down, start, size),
            0,
            slope_recv.at[n],
        ).wait_recv()
        piece[n, 1:2] = squares(start, size, total)
        if n == 0:
            meet_models()
        share_norm(n)

    def update_piece(n):
        kind, start, size = pieces[n]
        whole = whole_norm(n)
        ratio = jnp.sqrt(whole[0:1]) * (rate * learn_rate) * lax.rsqrt(
            whole[1:2] * (rate * rate) + 1e-06
        )
        if kind == "up":
            update_up(start, size, ratio)
        else:
            update_down(start, size, ratio)

    def update_up(start, size, ratio):
        spread[...] = jnp.broadcast_to(ratio, (LANES, LANES)).T
        per = size // UP_CUTS

        @pl.loop(0, size // per)
        def _(p):
            for q in range(per // ROWS):
                r = p * (per // ROWS) + q
                rows = pl.ds(start + r * ROWS, ROWS)
                scale = spread[pl.ds(r * ROWS, ROWS), :]
                for j in range(inner // LANES):
                    lanes = pl.ds(j * LANES, LANES)
                    new = next_up[rows, lanes] - sum_up(rows, lanes) * scale
                    next_up[rows, lanes] = new
                    half_up[pl.ds(mine + start + r * ROWS, ROWS), lanes] = new.astype(
                        jnp.bfloat16
                    )
            block = half_up.at[pl.ds(mine + start + p * per, per), :]
            pair_copy(block, block, 4, half_recv.at[0]).start()

    def update_down(start, size, ratio):
        scale = jnp.broadcast_to(ratio, (ROWS, LANES))
        lanes = pl.ds(start, size)
        place = pl.ds(mine + start, size)

        per = depth // DOWN_CUTS

        @pl.loop(0, DOWN_CUTS)
        def _(p):
            @pl.loop(0, per // down_rows)
            def _(r):
                for q in range(down_rows // ROWS):
                    rows = pl.ds(p * per + r * down_rows + q * ROWS, ROWS)
                    new = next_down[rows, lanes] - sum_down(rows, lanes) * scale
                    next_down[rows, lanes] = new
                    half_down[rows, place] = new.astype(jnp.bfloat16)

            block = half_down.at[pl.ds(p * per, per), place]
            pair_copy(block, block, 5, half_recv.at[1]).start()

    def update_norm():
        loads["slope norm"].wait()
        loads["param norm"].wait()
        for copy in norms:
            copy.wait_recv()
        sum_vec[...] = (
            (own_vec[...].astype(f32) + peer_vec[...].astype(f32)) * rate * learn_rate
        )
        new_gain = own_gain[...].reshape(1, share) - sum_vec[:, pl.ds(mine, share)]
        gain[:, pl.ds(mine, share)] = new_gain
        gain[:, pl.ds(theirs, share)] = (
            peer_gain[...].reshape(1, share) - sum_vec[:, pl.ds(theirs, share)]
        )
        next_norm[...] = new_gain.reshape(share)
        half_norm[...] = gain[...].reshape(half_norm.shape).astype(jnp.bfloat16)

    ahead = min(AHEAD, len(pieces))
    for n in range(len(pieces) + ahead):
        if n < len(pieces):
            measure_piece(n)
        if n >= ahead:
            update_piece(n - ahead)
    update_norm()

    for which, kind in enumerate(("up", "down")):
        pair_copy(
            peer_slope(kind, 0, share),
            cut(kind, peer_up, peer_down, 0, share),
            which,
            half_recv.at[which],
        ).wait_send()
        halves = pair_copy(
            half(kind, mine, share),
            half(kind, theirs, share),
            4 + which,
            half_recv.at[which],
        )
        halves.wait_send()
        halves.wait_recv()
    for copy in norms:
        copy.wait_send()
    norm_copy(got_piece, got_piece, 0, 1).wait_send()


def pieces_of(share):
    pieces = [("down", start, LANES) for start in range(0, share, LANES)]
    pieces += [("up", start, LANES) for start in range(0, share, LANES)]
    return pieces


def write_kernel(
    half_up,
    half_down,
    half_norm,
    next_up,
    next_down,
    next_norm,
    half_up_out,
    half_down_out,
    half_norm_out,
    next_up_out,
    next_down_out,
    next_norm_out,
    sem,
):
    moves = (
        (half_norm, half_norm_out),
        (next_norm, next_norm_out),
        (half_up, half_up_out),
        (half_down, half_down_out),
        (next_up, next_up_out),
        (next_down, next_down_out),
    )
    for i, (source, target) in enumerate(moves):
        cuts = 8 if len(source.shape) == 2 else 1
        rows = source.shape[0] // cuts
        for c in range(cuts):
            part = pl.ds(c * rows, rows)
            pltpu.make_async_copy(source.at[part], target.at[part], sem.at[i]).start()
    for i, (source, target) in enumerate(moves):
        pltpu.make_async_copy(source, target, sem.at[i]).wait()


def fused(replicas, models, slope_up, slope_down, slope_norm, param_up, param_down, param_norm):
    share, inner = param_up.shape
    depth = param_down.shape[0]
    width = slope_up.shape[1]
    count = len(pieces_of(share))
    bf16, f32 = jnp.bfloat16, jnp.float32
    hbm = pl.BlockSpec(memory_space=pltpu.HBM)
    vmem = pl.BlockSpec(memory_space=pltpu.VMEM)
    outs = pl.pallas_call(
        functools.partial(update_kernel, replicas, models),
        out_shape=(
            OUT((width, inner), bf16),
            OUT((depth, width), bf16),
            OUT((width,), bf16),
            OUT((share, inner), f32),
            OUT((depth, share), f32),
            OUT((share,), f32),
        ),
        in_specs=[hbm] * 6,
        out_specs=(vmem,) * 6,
        scratch_shapes=[
            pltpu.VMEM((share, inner), bf16),
            pltpu.VMEM((share, inner), bf16),
            pltpu.VMEM((depth, share), bf16),
            pltpu.VMEM((depth, share), bf16),
            pltpu.VMEM((1, width), bf16),
            pltpu.VMEM((1, width), bf16),
            pltpu.VMEM((share,), f32),
            pltpu.VMEM((share,), f32),
            pltpu.VMEM((1, width), f32),
            pltpu.VMEM((1, width), f32),
            pltpu.VMEM((count, 2, LANES), f32),
            pltpu.VMEM((count, models - 1, 2, LANES), f32),
            pltpu.VMEM((LANES, LANES), f32),
            pltpu.VMEM((LANES, LANES), f32),
            pltpu.SemaphoreType.DMA((8,)),
            pltpu.SemaphoreType.DMA((7,)),
            pltpu.SemaphoreType.DMA((count + 2,)),
            pltpu.SemaphoreType.DMA((2,)),
            pltpu.SemaphoreType.DMA((count,)),
            pltpu.SemaphoreType.REGULAR,
            pltpu.SemaphoreType.REGULAR,
        ],
        compiler_params=pltpu.CompilerParams(
            collective_id=0, has_side_effects=True, vmem_limit_bytes=24 * 2**20
        ),
    )(
        *(
            pltpu.with_memory_space_constraint(x, pltpu.HBM)
            for x in (
                slope_up, slope_down, slope_norm, param_up, param_down, param_norm
            )
        )
    )
    return pl.pallas_call(
        write_kernel,
        out_shape=(
            jax.ShapeDtypeStruct((width, inner), bf16),
            jax.ShapeDtypeStruct((depth, width), bf16),
            jax.ShapeDtypeStruct((width,), bf16),
            jax.ShapeDtypeStruct((share, inner), f32),
            jax.ShapeDtypeStruct((depth, share), f32),
            jax.ShapeDtypeStruct((share,), f32),
        ),
        in_specs=[vmem] * 6,
        out_specs=(hbm,) * 6,
        scratch_shapes=[pltpu.SemaphoreType.DMA((6,))],
        compiler_params=pltpu.CompilerParams(vmem_limit_bytes=24 * 2**20),
    )(*(pltpu.with_memory_space_constraint(x, pltpu.VMEM) for x in outs))


def suits(mesh, *arrays):
    slope_up, param_up, param_down = arrays
    return (
        mesh.shape["replica"] == 2
        and mesh.shape["model"] > 1
        and param_up.shape[0] % LANES == 0
        and param_up.shape[1] % LANES == 0
        and param_down.shape[0] % LANES == 0
    )


def step(mesh, slope_up, slope_down, slope_norm, param_up, param_down, param_norm):
    args = (slope_up, slope_down, slope_norm, param_up, param_down, param_norm)
    if suits(mesh, slope_up, param_up, param_down):
        return fused(mesh.shape["replica"], mesh.shape["model"], *args)
    return shards(*args)


OUT = pltpu.VMEM


def solution(mesh):
    return jax.shard_map(
        functools.partial(step, mesh),
        mesh=mesh,
        in_specs=(
            P(("copy", "replica"), None, "model"),
            P(("copy", "replica"), "model", None),
            P(("copy", "replica"), None),
            P(("copy", "replica"), "model"),
            P(("copy", "model"), "replica"),
            P(("copy", "replica")),
        ),
        out_specs=(
            P("copy", "model"),
            P(("copy", "model"), None),
            P("copy"),
            P(("copy", "replica"), "model"),
            P(("copy", "model"), "replica"),
            P(("copy", "replica")),
        ),
        check_vma=False,
    )
```

```python
import functools

import jax
import jax.numpy as jnp
from jax import lax
from jax.experimental import pallas as pl
from jax.experimental.pallas import tpu as pltpu
from jax.sharding import PartitionSpec as P

learn_rate = 0.5


def shards(slope_up, slope_down, slope_norm, param_up, param_down, param_norm):
    mean_up, mean_down = (
        lax.psum_scatter(
            slope_up[0].astype(jnp.float32).astype(jnp.bfloat16),
            "replica",
            scatter_dimension=0,
            tiled=True,
        ).astype(jnp.float32),
        lax.psum_scatter(
            slope_down[0].astype(jnp.float32).astype(jnp.bfloat16),
            "replica",
            scatter_dimension=1,
            tiled=True,
        ).astype(jnp.float32),
    )
    whole_norm = lax.psum(slope_norm[0].astype(jnp.float32), "replica")
    place = lax.axis_index("replica")
    mean_norm = lax.dynamic_slice_in_dim(
        whole_norm, place * param_norm.shape[0], param_norm.shape[0]
    )
    mean_rate = lax.axis_size("replica") ** (-0.5)
    mean_up = mean_up * mean_rate
    mean_down = mean_down * mean_rate
    mean_norm = mean_norm * mean_rate
    own_up, own_down, slope_up_norm, slope_down_norm = lax.psum(
        (
            jnp.sum(param_up * param_up, axis=1, keepdims=True),
            jnp.sum(param_down * param_down, axis=0, keepdims=True),
            jnp.sum(mean_up * mean_up, axis=1, keepdims=True),
            jnp.sum(mean_down * mean_down, axis=0, keepdims=True),
        ),
        "model",
    )
    mean_up = mean_up * (jnp.sqrt(own_up) * lax.rsqrt(slope_up_norm + 1e-06))
    mean_down = mean_down * (jnp.sqrt(own_down) * lax.rsqrt(slope_down_norm + 1e-06))
    next_up = param_up - learn_rate * mean_up
    next_down = param_down - learn_rate * mean_down
    next_norm = param_norm - learn_rate * mean_norm
    half_up, half_down, half_norm = (
        lax.all_gather(next_up.astype(jnp.bfloat16), "replica", axis=0, tiled=True),
        lax.all_gather(next_down.astype(jnp.bfloat16), "replica", axis=1, tiled=True),
        lax.all_gather(next_norm.astype(jnp.bfloat16), "replica", axis=0, tiled=True),
    )
    return (half_up, half_down, half_norm, next_up, next_down, next_norm)


MESH = pl.DeviceIdType.MESH
LANES = 128
ROWS = 32
AHEAD = 8
UP_CUTS = 2
DOWN_CUTS = 2


def update_kernel(
    replicas,
    models,
    slope_up,
    slope_down,
    slope_norm,
    param_up,
    param_down,
    param_norm,
    half_up,
    half_down,
    half_norm,
    next_up,
    next_down,
    next_norm,
    own_up,
    peer_up,
    own_down,
    peer_down,
    own_vec,
    peer_vec,
    own_gain,
    peer_gain,
    sum_vec,
    gain,
    lent_param,
    lent_slope,
    lent_own,
    lent_norm,
    piece,
    got_piece,
    square,
    spread,
    load_sem,
    send_sem,
    slope_recv,
    half_recv,
    piece_recv,
    lent_recv,
    pair_ready,
    model_ready,
):
    me = lax.axis_index("replica")
    other = 1 - me
    spot = lax.axis_index("model")
    share, inner = param_up.shape
    depth = param_down.shape[0]
    down_rows = 10 * ROWS
    mine = pl.multiple_of(me * share, LANES)
    theirs = pl.multiple_of(other * share, LANES)
    rate = replicas ** (-0.5)
    f32 = jnp.float32
    pieces = pieces_of(share)

    loads = {}

    def load(name, source, target):
        copy = pltpu.make_async_copy(source, target, load_sem.at[len(loads)])
        copy.start()
        loads[name] = copy

    def pair_copy(source, target, send, recv):
        return pltpu.make_async_remote_copy(
            source,
            target,
            send_sem.at[send],
            recv,
            device_id={"replica": other},
            device_id_type=MESH,
        )

    def own_slope(kind, start, size):
        if kind == "up":
            return slope_up.at[0, pl.ds(mine + start, size), :]
        return slope_down.at[0, :, pl.ds(mine + start, size)]

    def peer_slope(kind, start, size):
        if kind == "up":
            return slope_up.at[0, pl.ds(theirs + start, size), :]
        return slope_down.at[0, :, pl.ds(theirs + start, size)]

    def half(kind, start, size):
        if kind == "up":
            return half_up.at[pl.ds(start, size), :]
        return half_down.at[:, pl.ds(start, size)]

    def cut(kind, up, down, start, size):
        if kind == "up":
            return up.at[pl.ds(start, size), :]
        return down.at[:, pl.ds(start, size)]

    barrier = pltpu.get_barrier_semaphore()
    lead = me == replicas - 1

    @pl.when(lead)
    def _():
        pl.semaphore_signal(
            barrier, inc=1, device_id={"replica": other}, device_id_type=MESH
        )

    @pl.when(jnp.logical_not(lead))
    def _():
        pl.semaphore_wait(barrier, 1)
        pl.semaphore_signal(
            pair_ready, inc=1, device_id={"replica": other}, device_id_type=MESH
        )

    spare = share - LANES
    first = {}
    parts = [("down", 0, LANES), ("down", LANES, share - LANES), ("up", 0, share)]
    for span in parts:
        if span[2]:
            load(
                ("param", span),
                cut(span[0], param_up, param_down, *span[1:]),
                cut(span[0], next_up, next_down, *span[1:]),
            )
            load(
                ("slope", span),
                own_slope(*span),
                cut(span[0], own_up, own_down, *span[1:]),
            )
            for piece_span in pieces:
                if piece_span[0] == span[0] and piece_span[1] == span[1]:
                    first[piece_span] = span
    load("slope norm", slope_norm, own_vec)
    load("param norm", param_norm, own_gain)

    @pl.when(jnp.logical_and(spot == 0, lead))
    def _():
        pltpu.make_async_copy(
            peer_slope("up", spare, LANES), lent_own, load_sem.at[8]
        ).start()

    @pl.when(lead)
    def _():
        pl.semaphore_wait(pair_ready, 1)
        for k in range(1, models):
            pl.semaphore_signal(
                barrier,
                inc=1,
                device_id={"model": lax.rem(spot + k, models)},
                device_id_type=MESH,
            )

    def meet_models():
        @pl.when(lead)
        def _():
            pl.semaphore_wait(barrier, models - 1)
            pl.semaphore_signal(
                model_ready, inc=1, device_id={"replica": other}, device_id_type=MESH
            )

        @pl.when(jnp.logical_not(lead))
        def _():
            pl.semaphore_wait(model_ready, 1)

    for n, span in enumerate(pieces):
        pair_copy(
            peer_slope(*span),
            cut(span[0], peer_up, peer_down, *span[1:]),
            0 if span[0] == "up" else 1,
            slope_recv.at[n],
        ).start()
    norms = [
        pair_copy(slope_norm, peer_vec, 2, slope_recv.at[len(pieces)]),
        pair_copy(param_norm, peer_gain, 3, slope_recv.at[len(pieces) + 1]),
    ]
    for copy in norms:
        copy.start()

    last = len(pieces) - 1
    gives = jnp.logical_and(spot == 0, jnp.logical_not(lead))
    takes = jnp.logical_and(spot == 0, lead)
    lent = (
        pair_copy(param_up.at[pl.ds(spare, LANES), :], lent_param, 8, lent_recv.at[0]),
        pair_copy(own_slope("up", spare, LANES), lent_slope, 9, lent_recv.at[1]),
    )
    @pl.when(gives)
    def _():
        for copy in lent:
            copy.start()

    def norm_copy(source, target, n, k):
        return pltpu.make_async_remote_copy(
            source,
            target,
            send_sem.at[6],
            piece_recv.at[n],
            device_id={"model": lax.rem(spot + k, models)},
            device_id_type=MESH,
        )

    def share_norm(n):
        for k in range(1, models):
            norm_copy(piece.at[n], got_piece.at[n, k - 1], n, k).start()

    def lend_norm(source, target):
        return pltpu.make_async_remote_copy(
            source,
            target,
            send_sem.at[7],
            lent_recv.at[2],
            device_id={"model": 0, "replica": other},
            device_id_type=MESH,
        )

    def whole_norm(n):
        norm_copy(got_piece.at[n], got_piece.at[n], n, 1).wait_recv()
        total = piece[n]
        for k in range(1, models):
            total = total + got_piece[n, k - 1]
        return total

    def ratio_of(whole):
        return jnp.sqrt(whole[0:1]) * (rate * learn_rate) * lax.rsqrt(
            whole[1:2] * (rate * rate) + 1e-06
        )

    square[...] = jnp.zeros(square.shape, f32)

    def row_squares(start, size, value):
        for r in range(size // ROWS):
            rows = pl.ds(start + r * ROWS, ROWS)
            total = jnp.zeros((ROWS, LANES), f32)
            for j in range(inner // LANES):
                x = value(rows, pl.ds(j * LANES, LANES))
                total = total + x * x
            square[pl.ds(r * ROWS, ROWS), :] = total

        return jnp.sum(square[...].T, axis=0, keepdims=True)

    def column_squares(start, size, value):
        def body(r, total):
            for q in range(down_rows // ROWS):
                x = value(pl.ds(r * down_rows + q * ROWS, ROWS), pl.ds(start, size))
                total = total + x * x
            return total

        total = lax.fori_loop(
            0, depth // down_rows, body, jnp.zeros((ROWS, LANES), f32)
        )
        return jnp.sum(total, axis=0, keepdims=True)

    def sum_up(rows, lanes):
        return own_up[rows, lanes].astype(f32) + peer_up[rows, lanes].astype(f32)

    def sum_down(rows, lanes):
        return own_down[rows, lanes].astype(f32) + peer_down[rows, lanes].astype(f32)

    def measure_piece(n):
        kind, start, size = pieces[n]
        squares = row_squares if kind == "up" else column_squares
        param = next_up if kind == "up" else next_down
        total = sum_up if kind == "up" else sum_down
        span = first.get(pieces[n])
        if span:
            loads["param", span].wait()
        piece[n, 0:1] = squares(start, size, lambda rows, lanes: param[rows, lanes])
        if span:
            loads["slope", span].wait()
        pair_copy(
            peer_slope(*pieces[n]),
            cut(kind, peer_up, peer_down, start, size),
            0,
            slope_recv.at[n],
        ).wait_recv()
        piece[n, 1:2] = squares(start, size, total)
        if n == 0:
            meet_models()
        share_norm(n)
        if n == last:

            @pl.when(jnp.logical_not(lead))
            def _():
                lend_norm(piece.at[n], lent_norm.at[models - 1 - spot]).start()

    def update_piece(n):
        kind, start, size = pieces[n]
        ratio = ratio_of(whole_norm(n))
        if kind == "up":
            update_up(start, size, ratio)
        else:
            update_down(start, size, ratio)

    def update_up(start, size, ratio):
        spread[...] = jnp.broadcast_to(ratio, (LANES, LANES)).T
        per = size // UP_CUTS

        @pl.loop(0, size // per)
        def _(p):
            for q in range(per // ROWS):
                r = p * (per // ROWS) + q
                rows = pl.ds(start + r * ROWS, ROWS)
                scale = spread[pl.ds(r * ROWS, ROWS), :]
                for j in range(inner // LANES):
                    lanes = pl.ds(j * LANES, LANES)
                    new = next_up[rows, lanes] - sum_up(rows, lanes) * scale
                    next_up[rows, lanes] = new
                    half_up[pl.ds(mine + start + r * ROWS, ROWS), lanes] = new.astype(
                        jnp.bfloat16
                    )
            def push_half():
                block = half_up.at[pl.ds(mine + start + p * per, per), :]
                pair_copy(block, block, 4, half_recv.at[0]).start()

            if start == spare:
                pl.when(jnp.logical_not(gives))(push_half)
            else:
                push_half()

    def update_down(start, size, ratio):
        scale = jnp.broadcast_to(ratio, (ROWS, LANES))
        lanes = pl.ds(start, size)
        place = pl.ds(mine + start, size)

        per = depth // DOWN_CUTS

        @pl.loop(0, DOWN_CUTS)
        def _(p):
            @pl.loop(0, per // down_rows)
            def _(r):
                for q in range(down_rows // ROWS):
                    rows = pl.ds(p * per + r * down_rows + q * ROWS, ROWS)
                    new = next_down[rows, lanes] - sum_down(rows, lanes) * scale
                    next_down[rows, lanes] = new
                    half_down[rows, place] = new.astype(jnp.bfloat16)

            block = half_down.at[pl.ds(p * per, per), place]
            pair_copy(block, block, 5, half_recv.at[1]).start()

    def update_norm():
        loads["slope norm"].wait()
        loads["param norm"].wait()
        for copy in norms:
            copy.wait_recv()
        sum_vec[...] = (
            (own_vec[...].astype(f32) + peer_vec[...].astype(f32)) * rate * learn_rate
        )
        new_gain = own_gain[...].reshape(1, share) - sum_vec[:, pl.ds(mine, share)]
        gain[:, pl.ds(mine, share)] = new_gain
        gain[:, pl.ds(theirs, share)] = (
            peer_gain[...].reshape(1, share) - sum_vec[:, pl.ds(theirs, share)]
        )
        next_norm[...] = new_gain.reshape(share)
        half_norm[...] = gain[...].reshape(half_norm.shape).astype(jnp.bfloat16)

    ahead = min(AHEAD, len(pieces))
    for n in range(len(pieces) + ahead):
        if n < len(pieces):
            measure_piece(n)
        if n >= ahead:
            update_piece(n - ahead)
    update_norm()

    @pl.when(takes)
    def _():
        for copy in lent:
            copy.wait_recv()
        pltpu.make_async_copy(
            peer_slope("up", spare, LANES), lent_own, load_sem.at[8]
        ).wait()
        lend_norm(lent_norm, lent_norm).wait_recv()
        whole = lent_norm[models - 1]
        for k in range(1, models):
            whole = whole + lent_norm[k - 1]
        spread[...] = jnp.broadcast_to(ratio_of(whole), (LANES, LANES)).T

        @pl.loop(0, LANES // ROWS)
        def _(r):
            rows = pl.ds(r * ROWS, ROWS)
            scale = spread[rows, :]
            for j in range(inner // LANES):
                lanes = pl.ds(j * LANES, LANES)
                total = lent_slope[rows, lanes].astype(f32) + lent_own[
                    rows, lanes
                ].astype(f32)
                half_up[pl.ds(theirs + spare + r * ROWS, ROWS), lanes] = (
                    lent_param[rows, lanes] - total * scale
                ).astype(jnp.bfloat16)

    for which, kind in enumerate(("up", "down")):
        pair_copy(
            peer_slope(kind, 0, share),
            cut(kind, peer_up, peer_down, 0, share),
            which,
            half_recv.at[which],
        ).wait_send()

        def halves(size):
            return pair_copy(
                half(kind, mine, size),
                half(kind, theirs, size),
                4 + which,
                half_recv.at[which],
            )

        if kind == "up":

            @pl.when(gives)
            def _():
                halves(spare).wait_send()
                for copy in lent:
                    copy.wait_send()

            @pl.when(jnp.logical_not(gives))
            def _():
                halves(share).wait_send()

            @pl.when(takes)
            def _():
                halves(spare).wait_recv()

            @pl.when(jnp.logical_not(takes))
            def _():
                halves(share).wait_recv()

        else:
            halves(share).wait_send()
            halves(share).wait_recv()

    @pl.when(jnp.logical_not(lead))
    def _():
        lend_norm(piece.at[last], lent_norm.at[0]).wait_send()

    for copy in norms:
        copy.wait_send()
    norm_copy(got_piece, got_piece, 0, 1).wait_send()


def pieces_of(share):
    pieces = [("down", start, LANES) for start in range(0, share, LANES)]
    pieces += [("up", start, LANES) for start in range(0, share, LANES)]
    return pieces


def write_kernel(
    half_up,
    half_down,
    half_norm,
    next_up,
    next_down,
    next_norm,
    half_up_out,
    half_down_out,
    half_norm_out,
    next_up_out,
    next_down_out,
    next_norm_out,
    sem,
):
    moves = (
        (half_norm, half_norm_out),
        (next_norm, next_norm_out),
        (half_up, half_up_out),
        (half_down, half_down_out),
        (next_up, next_up_out),
        (next_down, next_down_out),
    )
    for i, (source, target) in enumerate(moves):
        cuts = 8 if len(source.shape) == 2 else 1
        rows = source.shape[0] // cuts
        for c in range(cuts):
            part = pl.ds(c * rows, rows)
            pltpu.make_async_copy(source.at[part], target.at[part], sem.at[i]).start()
    for i, (source, target) in enumerate(moves):
        pltpu.make_async_copy(source, target, sem.at[i]).wait()


def fused(replicas, models, slope_up, slope_down, slope_norm, param_up, param_down, param_norm):
    share, inner = param_up.shape
    depth = param_down.shape[0]
    width = slope_up.shape[1]
    count = len(pieces_of(share))
    bf16, f32 = jnp.bfloat16, jnp.float32
    hbm = pl.BlockSpec(memory_space=pltpu.HBM)
    vmem = pl.BlockSpec(memory_space=pltpu.VMEM)
    outs = pl.pallas_call(
        functools.partial(update_kernel, replicas, models),
        out_shape=(
            OUT((width, inner), bf16),
            OUT((depth, width), bf16),
            OUT((width,), bf16),
            OUT((share, inner), f32),
            OUT((depth, share), f32),
            OUT((share,), f32),
        ),
        in_specs=[hbm] * 6,
        out_specs=(vmem,) * 6,
        scratch_shapes=[
            pltpu.VMEM((share, inner), bf16),
            pltpu.VMEM((share, inner), bf16),
            pltpu.VMEM((depth, share), bf16),
            pltpu.VMEM((depth, share), bf16),
            pltpu.VMEM((1, width), bf16),
            pltpu.VMEM((1, width), bf16),
            pltpu.VMEM((share,), f32),
            pltpu.VMEM((share,), f32),
            pltpu.VMEM((1, width), f32),
            pltpu.VMEM((1, width), f32),
            pltpu.VMEM((LANES, inner), f32),
            pltpu.VMEM((LANES, inner), bf16),
            pltpu.VMEM((LANES, inner), bf16),
            pltpu.VMEM((models, 2, LANES), f32),
            pltpu.VMEM((count, 2, LANES), f32),
            pltpu.VMEM((count, models - 1, 2, LANES), f32),
            pltpu.VMEM((LANES, LANES), f32),
            pltpu.VMEM((LANES, LANES), f32),
            pltpu.SemaphoreType.DMA((9,)),
            pltpu.SemaphoreType.DMA((10,)),
            pltpu.SemaphoreType.DMA((count + 2,)),
            pltpu.SemaphoreType.DMA((2,)),
            pltpu.SemaphoreType.DMA((count,)),
            pltpu.SemaphoreType.DMA((3,)),
            pltpu.SemaphoreType.REGULAR,
            pltpu.SemaphoreType.REGULAR,
        ],
        compiler_params=pltpu.CompilerParams(
            collective_id=0, has_side_effects=True, vmem_limit_bytes=24 * 2**20
        ),
    )(
        *(
            pltpu.with_memory_space_constraint(x, pltpu.HBM)
            for x in (
                slope_up, slope_down, slope_norm, param_up, param_down, param_norm
            )
        )
    )
    return pl.pallas_call(
        write_kernel,
        out_shape=(
            jax.ShapeDtypeStruct((width, inner), bf16),
            jax.ShapeDtypeStruct((depth, width), bf16),
            jax.ShapeDtypeStruct((width,), bf16),
            jax.ShapeDtypeStruct((share, inner), f32),
            jax.ShapeDtypeStruct((depth, share), f32),
            jax.ShapeDtypeStruct((share,), f32),
        ),
        in_specs=[vmem] * 6,
        out_specs=(hbm,) * 6,
        scratch_shapes=[pltpu.SemaphoreType.DMA((6,))],
        compiler_params=pltpu.CompilerParams(vmem_limit_bytes=24 * 2**20),
    )(*(pltpu.with_memory_space_constraint(x, pltpu.VMEM) for x in outs))


def suits(mesh, *arrays):
    slope_up, param_up, param_down = arrays
    return (
        mesh.shape["replica"] == 2
        and mesh.shape["model"] > 1
        and param_up.shape[0] % LANES == 0
        and param_up.shape[0] > LANES
        and param_up.shape[1] % LANES == 0
        and param_down.shape[0] % LANES == 0
    )


def step(mesh, slope_up, slope_down, slope_norm, param_up, param_down, param_norm):
    args = (slope_up, slope_down, slope_norm, param_up, param_down, param_norm)
    if suits(mesh, slope_up, param_up, param_down):
        return fused(mesh.shape["replica"], mesh.shape["model"], *args)
    return shards(*args)


OUT = pltpu.VMEM


def solution(mesh):
    return jax.shard_map(
        functools.partial(step, mesh),
        mesh=mesh,
        in_specs=(
            P(("copy", "replica"), None, "model"),
            P(("copy", "replica"), "model", None),
            P(("copy", "replica"), None),
            P(("copy", "replica"), "model"),
            P(("copy", "model"), "replica"),
            P(("copy", "replica")),
        ),
        out_specs=(
            P("copy", "model"),
            P(("copy", "model"), None),
            P("copy"),
            P(("copy", "replica"), "model"),
            P(("copy", "model"), "replica"),
            P(("copy", "replica")),
        ),
        check_vma=False,
    )
```

```python
import functools

import jax
import jax.numpy as jnp
from jax import lax
from jax.experimental import pallas as pl
from jax.experimental.pallas import tpu as pltpu
from jax.sharding import PartitionSpec as P

learn_rate = 0.5


def shards(slope_up, slope_down, slope_norm, param_up, param_down, param_norm):
    mean_up, mean_down = (
        lax.psum_scatter(
            slope_up[0].astype(jnp.float32).astype(jnp.bfloat16),
            "replica",
            scatter_dimension=0,
            tiled=True,
        ).astype(jnp.float32),
        lax.psum_scatter(
            slope_down[0].astype(jnp.float32).astype(jnp.bfloat16),
            "replica",
            scatter_dimension=1,
            tiled=True,
        ).astype(jnp.float32),
    )
    whole_norm = lax.psum(slope_norm[0].astype(jnp.float32), "replica")
    place = lax.axis_index("replica")
    mean_norm = lax.dynamic_slice_in_dim(
        whole_norm, place * param_norm.shape[0], param_norm.shape[0]
    )
    mean_rate = lax.axis_size("replica") ** (-0.5)
    mean_up = mean_up * mean_rate
    mean_down = mean_down * mean_rate
    mean_norm = mean_norm * mean_rate
    own_up, own_down, slope_up_norm, slope_down_norm = lax.psum(
        (
            jnp.sum(param_up * param_up, axis=1, keepdims=True),
            jnp.sum(param_down * param_down, axis=0, keepdims=True),
            jnp.sum(mean_up * mean_up, axis=1, keepdims=True),
            jnp.sum(mean_down * mean_down, axis=0, keepdims=True),
        ),
        "model",
    )
    mean_up = mean_up * (jnp.sqrt(own_up) * lax.rsqrt(slope_up_norm + 1e-06))
    mean_down = mean_down * (jnp.sqrt(own_down) * lax.rsqrt(slope_down_norm + 1e-06))
    next_up = param_up - learn_rate * mean_up
    next_down = param_down - learn_rate * mean_down
    next_norm = param_norm - learn_rate * mean_norm
    half_up, half_down, half_norm = (
        lax.all_gather(next_up.astype(jnp.bfloat16), "replica", axis=0, tiled=True),
        lax.all_gather(next_down.astype(jnp.bfloat16), "replica", axis=1, tiled=True),
        lax.all_gather(next_norm.astype(jnp.bfloat16), "replica", axis=0, tiled=True),
    )
    return (half_up, half_down, half_norm, next_up, next_down, next_norm)


MESH = pl.DeviceIdType.MESH
LANES = 128
ROWS = 32
AHEAD = 8
UP_CUTS = 2
DOWN_CUTS = 4


def update_kernel(
    replicas,
    models,
    slope_up,
    slope_down,
    slope_norm,
    param_up,
    param_down,
    param_norm,
    half_up,
    half_down,
    half_norm,
    next_up,
    next_down,
    next_norm,
    own_up,
    peer_up,
    own_down,
    peer_down,
    own_vec,
    peer_vec,
    own_gain,
    peer_gain,
    sum_vec,
    gain,
    lent_param,
    lent_slope,
    lent_own,
    lent_norm,
    piece,
    got_piece,
    square,
    spread,
    load_sem,
    send_sem,
    slope_recv,
    half_recv,
    piece_recv,
    lent_recv,
    pair_ready,
    model_ready,
):
    me = lax.axis_index("replica")
    other = 1 - me
    spot = lax.axis_index("model")
    share, inner = param_up.shape
    depth = param_down.shape[0]
    down_per, down_rows = steps_of(depth)
    mine = pl.multiple_of(me * share, LANES)
    theirs = pl.multiple_of(other * share, LANES)
    rate = replicas ** (-0.5)
    f32 = jnp.float32
    pieces = pieces_of(share)

    loads = {}

    def load(name, source, target):
        copy = pltpu.make_async_copy(source, target, load_sem.at[len(loads)])
        copy.start()
        loads[name] = copy

    def pair_copy(source, target, send, recv):
        return pltpu.make_async_remote_copy(
            source,
            target,
            send_sem.at[send],
            recv,
            device_id={"replica": other},
            device_id_type=MESH,
        )

    def own_slope(kind, start, size):
        if kind == "up":
            return slope_up.at[0, pl.ds(mine + start, size), :]
        return slope_down.at[0, :, pl.ds(mine + start, size)]

    def peer_slope(kind, start, size):
        if kind == "up":
            return slope_up.at[0, pl.ds(theirs + start, size), :]
        return slope_down.at[0, :, pl.ds(theirs + start, size)]

    def half(kind, start, size):
        if kind == "up":
            return half_up.at[pl.ds(start, size), :]
        return half_down.at[:, pl.ds(start, size)]

    def cut(kind, up, down, start, size):
        if kind == "up":
            return up.at[pl.ds(start, size), :]
        return down.at[:, pl.ds(start, size)]

    barrier = pltpu.get_barrier_semaphore()
    lead = me == replicas - 1

    @pl.when(lead)
    def _():
        pl.semaphore_signal(
            barrier, inc=1, device_id={"replica": other}, device_id_type=MESH
        )

    @pl.when(jnp.logical_not(lead))
    def _():
        pl.semaphore_wait(barrier, 1)
        pl.semaphore_signal(
            pair_ready, inc=1, device_id={"replica": other}, device_id_type=MESH
        )

    spare = share - LANES
    first = {}
    parts = [("down", 0, LANES), ("down", LANES, share - LANES), ("up", 0, share)]
    for span in parts:
        if span[2]:
            load(
                ("param", span),
                cut(span[0], param_up, param_down, *span[1:]),
                cut(span[0], next_up, next_down, *span[1:]),
            )
            load(
                ("slope", span),
                own_slope(*span),
                cut(span[0], own_up, own_down, *span[1:]),
            )
            for piece_span in pieces:
                if piece_span[0] == span[0] and piece_span[1] == span[1]:
                    first[piece_span] = span
    load("slope norm", slope_norm, own_vec)
    load("param norm", param_norm, own_gain)

    @pl.when(jnp.logical_and(spot == 0, lead))
    def _():
        pltpu.make_async_copy(
            peer_slope("up", spare, LANES), lent_own, load_sem.at[8]
        ).start()

    @pl.when(lead)
    def _():
        pl.semaphore_wait(pair_ready, 1)
        for k in range(1, models):
            pl.semaphore_signal(
                barrier,
                inc=1,
                device_id={"model": lax.rem(spot + k, models)},
                device_id_type=MESH,
            )

    def meet_models():
        @pl.when(lead)
        def _():
            pl.semaphore_wait(barrier, models - 1)
            pl.semaphore_signal(
                model_ready, inc=1, device_id={"replica": other}, device_id_type=MESH
            )

        @pl.when(jnp.logical_not(lead))
        def _():
            pl.semaphore_wait(model_ready, 1)

    for n, span in enumerate(pieces):
        pair_copy(
            peer_slope(*span),
            cut(span[0], peer_up, peer_down, *span[1:]),
            0,
            slope_recv.at[n],
        ).start()
    norms = [
        pair_copy(slope_norm, peer_vec, 1, slope_recv.at[len(pieces)]),
        pair_copy(param_norm, peer_gain, 2, slope_recv.at[len(pieces) + 1]),
    ]
    for copy in norms:
        copy.start()

    last = len(pieces) - 1
    gives = jnp.logical_and(spot == 0, jnp.logical_not(lead))
    takes = jnp.logical_and(spot == 0, lead)
    lent = (
        pair_copy(param_up.at[pl.ds(spare, LANES), :], lent_param, 6, lent_recv.at[0]),
        pair_copy(own_slope("up", spare, LANES), lent_slope, 6, lent_recv.at[0]),
    )
    both = next_up.at[pl.ds(0, LANES + LANES // 2), :]
    lent_both = pair_copy(both, both, 6, lent_recv.at[0])

    @pl.when(gives)
    def _():
        for copy in lent:
            copy.start()

    def norm_copy(source, target, n, k):
        return pltpu.make_async_remote_copy(
            source,
            target,
            send_sem.at[4],
            piece_recv.at[n],
            device_id={"model": lax.rem(spot + k, models)},
            device_id_type=MESH,
        )

    def share_norm(n):
        for k in range(1, models):
            norm_copy(piece.at[n], got_piece.at[n, k - 1], n, k).start()

    def lend_norm(source, target):
        return pltpu.make_async_remote_copy(
            source,
            target,
            send_sem.at[5],
            lent_recv.at[1],
            device_id={"model": 0, "replica": other},
            device_id_type=MESH,
        )

    def whole_norm(n):
        norm_copy(got_piece.at[n], got_piece.at[n], n, 1).wait_recv()
        total = piece[n]
        for k in range(1, models):
            total = total + got_piece[n, k - 1]
        return total

    def ratio_of(whole):
        return jnp.sqrt(whole[0:1]) * (rate * learn_rate) * lax.rsqrt(
            whole[1:2] * (rate * rate) + 1e-06
        )

    square[...] = jnp.zeros(square.shape, f32)

    def row_squares(start, size, value):
        for r in range(size // ROWS):
            rows = pl.ds(start + r * ROWS, ROWS)
            total = jnp.zeros((ROWS, LANES), f32)
            for j in range(inner // LANES):
                x = value(rows, pl.ds(j * LANES, LANES))
                total = total + x * x
            square[pl.ds(r * ROWS, ROWS), :] = total

        return jnp.sum(square[...].T, axis=0, keepdims=True)

    def column_squares(start, size, value):
        def body(r, total):
            for q in range(down_rows // ROWS):
                x = value(pl.ds(r * down_rows + q * ROWS, ROWS), pl.ds(start, size))
                total = total + x * x
            return total

        total = lax.fori_loop(
            0, depth // down_rows, body, jnp.zeros((ROWS, LANES), f32)
        )
        return jnp.sum(total, axis=0, keepdims=True)

    def sum_up(rows, lanes):
        return own_up[rows, lanes].astype(f32) + peer_up[rows, lanes].astype(f32)

    def sum_down(rows, lanes):
        return own_down[rows, lanes].astype(f32) + peer_down[rows, lanes].astype(f32)

    def measure_piece(n):
        kind, start, size = pieces[n]
        squares = row_squares if kind == "up" else column_squares
        param = next_up if kind == "up" else next_down
        total = sum_up if kind == "up" else sum_down
        span = first.get(pieces[n])
        if span:
            loads["param", span].wait()
        piece[n, 0:1] = squares(start, size, lambda rows, lanes: param[rows, lanes])
        if span:
            loads["slope", span].wait()
        pair_copy(
            peer_slope(*pieces[n]),
            cut(kind, peer_up, peer_down, start, size),
            0,
            slope_recv.at[n],
        ).wait_recv()
        piece[n, 1:2] = squares(start, size, total)
        if n == 0:
            meet_models()
        share_norm(n)
        if n == last:

            @pl.when(jnp.logical_not(lead))
            def _():
                lend_norm(piece.at[n], lent_norm.at[models - 1 - spot]).start()

    def update_piece(n):
        kind, start, size = pieces[n]
        ratio = ratio_of(whole_norm(n))
        if kind == "up":
            update_up(start, size, ratio)
        else:
            update_down(start, size, ratio)

    def update_up(start, size, ratio):
        spread[...] = jnp.broadcast_to(ratio, (LANES, LANES)).T
        per = size // UP_CUTS

        @pl.loop(0, size // per)
        def _(p):
            for q in range(per // ROWS):
                r = p * (per // ROWS) + q
                rows = pl.ds(start + r * ROWS, ROWS)
                scale = spread[pl.ds(r * ROWS, ROWS), :]
                for j in range(inner // LANES):
                    lanes = pl.ds(j * LANES, LANES)
                    new = next_up[rows, lanes] - sum_up(rows, lanes) * scale
                    next_up[rows, lanes] = new
                    half_up[pl.ds(mine + start + r * ROWS, ROWS), lanes] = new.astype(
                        jnp.bfloat16
                    )
            def push_half():
                block = half_up.at[pl.ds(mine + start + p * per, per), :]
                pair_copy(block, block, 3, half_recv.at[0]).start()

            if start == spare:
                pl.when(jnp.logical_not(gives))(push_half)
            else:
                push_half()

    def update_down(start, size, ratio):
        scale = jnp.broadcast_to(ratio, (ROWS, LANES))
        lanes = pl.ds(start, size)
        place = pl.ds(mine + start, size)

        per = down_per

        @pl.loop(0, depth // per)
        def _(p):
            @pl.loop(0, per // down_rows)
            def _(r):
                for q in range(down_rows // ROWS):
                    rows = pl.ds(p * per + r * down_rows + q * ROWS, ROWS)
                    new = next_down[rows, lanes] - sum_down(rows, lanes) * scale
                    next_down[rows, lanes] = new
                    half_down[rows, place] = new.astype(jnp.bfloat16)

            block = half_down.at[pl.ds(p * per, per), place]
            pair_copy(block, block, 3, half_recv.at[0]).start()

    def update_norm():
        loads["slope norm"].wait()
        loads["param norm"].wait()
        for copy in norms:
            copy.wait_recv()
        sum_vec[...] = (
            (own_vec[...].astype(f32) + peer_vec[...].astype(f32)) * rate * learn_rate
        )
        new_gain = own_gain[...].reshape(1, share) - sum_vec[:, pl.ds(mine, share)]
        gain[:, pl.ds(mine, share)] = new_gain
        gain[:, pl.ds(theirs, share)] = (
            peer_gain[...].reshape(1, share) - sum_vec[:, pl.ds(theirs, share)]
        )
        next_norm[...] = new_gain.reshape(share)
        half_norm[...] = gain[...].reshape(half_norm.shape).astype(jnp.bfloat16)

    ahead = min(AHEAD, len(pieces))
    for n in range(len(pieces) + ahead):
        if n < len(pieces):
            measure_piece(n)
        if n >= ahead:
            update_piece(n - ahead)
    update_norm()

    @pl.when(takes)
    def _():
        lent_both.wait_recv()
        pltpu.make_async_copy(
            peer_slope("up", spare, LANES), lent_own, load_sem.at[8]
        ).wait()
        lend_norm(lent_norm, lent_norm).wait_recv()
        whole = lent_norm[models - 1]
        for k in range(1, models):
            whole = whole + lent_norm[k - 1]
        spread[...] = jnp.broadcast_to(ratio_of(whole), (LANES, LANES)).T

        @pl.loop(0, LANES // ROWS)
        def _(r):
            rows = pl.ds(r * ROWS, ROWS)
            scale = spread[rows, :]
            for j in range(inner // LANES):
                lanes = pl.ds(j * LANES, LANES)
                total = lent_slope[rows, lanes].astype(f32) + lent_own[
                    rows, lanes
                ].astype(f32)
                half_up[pl.ds(theirs + spare + r * ROWS, ROWS), lanes] = (
                    lent_param[rows, lanes] - total * scale
                ).astype(jnp.bfloat16)

    pair_copy(half_up, half_up, 0, half_recv.at[0]).wait_send()

    def halves(rows):
        block = half_up.at[pl.ds(0, rows), :]
        return pair_copy(block, block, 3, half_recv.at[0])

    @pl.when(gives)
    def _():
        halves(2 * share - LANES).wait_send()
        lent_both.wait_send()

    @pl.when(jnp.logical_not(gives))
    def _():
        halves(2 * share).wait_send()

    @pl.when(takes)
    def _():
        halves(2 * share - LANES).wait_recv()

    @pl.when(jnp.logical_not(takes))
    def _():
        halves(2 * share).wait_recv()

    @pl.when(jnp.logical_not(lead))
    def _():
        lend_norm(piece.at[last], lent_norm.at[0]).wait_send()

    for copy in norms:
        copy.wait_send()
    norm_copy(got_piece, got_piece, 0, 1).wait_send()


def steps_of(depth):
    cuts = max(c for c in range(1, DOWN_CUTS + 1) if depth % (c * ROWS) == 0)
    per = depth // cuts
    return per, max(k * ROWS for k in range(1, 11) if per % (k * ROWS) == 0)


def pieces_of(share):
    pieces = [("down", start, LANES) for start in range(0, share, LANES)]
    pieces += [("up", start, LANES) for start in range(0, share, LANES)]
    return pieces


def write_kernel(
    half_up,
    half_down,
    half_norm,
    next_up,
    next_down,
    next_norm,
    half_up_out,
    half_down_out,
    half_norm_out,
    next_up_out,
    next_down_out,
    next_norm_out,
    sem,
):
    moves = (
        (half_norm, half_norm_out),
        (next_norm, next_norm_out),
        (half_up, half_up_out),
        (half_down, half_down_out),
        (next_up, next_up_out),
        (next_down, next_down_out),
    )
    for i, (source, target) in enumerate(moves):
        cuts = 8 if len(source.shape) == 2 else 1
        rows = source.shape[0] // cuts
        for c in range(cuts):
            part = pl.ds(c * rows, rows)
            pltpu.make_async_copy(source.at[part], target.at[part], sem.at[i]).start()
    for i, (source, target) in enumerate(moves):
        pltpu.make_async_copy(source, target, sem.at[i]).wait()


def fused(replicas, models, slope_up, slope_down, slope_norm, param_up, param_down, param_norm):
    share, inner = param_up.shape
    depth = param_down.shape[0]
    width = slope_up.shape[1]
    count = len(pieces_of(share))
    bf16, f32 = jnp.bfloat16, jnp.float32
    hbm = pl.BlockSpec(memory_space=pltpu.HBM)
    vmem = pl.BlockSpec(memory_space=pltpu.VMEM)
    outs = pl.pallas_call(
        functools.partial(update_kernel, replicas, models),
        out_shape=(
            OUT((width, inner), bf16),
            OUT((depth, width), bf16),
            OUT((width,), bf16),
            OUT((share, inner), f32),
            OUT((depth, share), f32),
            OUT((share,), f32),
        ),
        in_specs=[hbm] * 6,
        out_specs=(vmem,) * 6,
        scratch_shapes=[
            pltpu.VMEM((share, inner), bf16),
            pltpu.VMEM((share, inner), bf16),
            pltpu.VMEM((depth, share), bf16),
            pltpu.VMEM((depth, share), bf16),
            pltpu.VMEM((1, width), bf16),
            pltpu.VMEM((1, width), bf16),
            pltpu.VMEM((share,), f32),
            pltpu.VMEM((share,), f32),
            pltpu.VMEM((1, width), f32),
            pltpu.VMEM((1, width), f32),
            pltpu.VMEM((LANES, inner), f32),
            pltpu.VMEM((LANES, inner), bf16),
            pltpu.VMEM((LANES, inner), bf16),
            pltpu.VMEM((models, 2, LANES), f32),
            pltpu.VMEM((count, 2, LANES), f32),
            pltpu.VMEM((count, models - 1, 2, LANES), f32),
            pltpu.VMEM((LANES, LANES), f32),
            pltpu.VMEM((LANES, LANES), f32),
            pltpu.SemaphoreType.DMA((9,)),
            pltpu.SemaphoreType.DMA((7,)),
            pltpu.SemaphoreType.DMA((count + 2,)),
            pltpu.SemaphoreType.DMA((1,)),
            pltpu.SemaphoreType.DMA((count,)),
            pltpu.SemaphoreType.DMA((2,)),
            pltpu.SemaphoreType.REGULAR,
            pltpu.SemaphoreType.REGULAR,
        ],
        compiler_params=pltpu.CompilerParams(
            collective_id=0, has_side_effects=True, vmem_limit_bytes=24 * 2**20
        ),
    )(
        *(
            pltpu.with_memory_space_constraint(x, pltpu.HBM)
            for x in (
                slope_up, slope_down, slope_norm, param_up, param_down, param_norm
            )
        )
    )
    return pl.pallas_call(
        write_kernel,
        out_shape=(
            jax.ShapeDtypeStruct((width, inner), bf16),
            jax.ShapeDtypeStruct((depth, width), bf16),
            jax.ShapeDtypeStruct((width,), bf16),
            jax.ShapeDtypeStruct((share, inner), f32),
            jax.ShapeDtypeStruct((depth, share), f32),
            jax.ShapeDtypeStruct((share,), f32),
        ),
        in_specs=[vmem] * 6,
        out_specs=(hbm,) * 6,
        scratch_shapes=[pltpu.SemaphoreType.DMA((6,))],
        compiler_params=pltpu.CompilerParams(vmem_limit_bytes=24 * 2**20),
    )(*(pltpu.with_memory_space_constraint(x, pltpu.VMEM) for x in outs))


def suits(mesh, *arrays):
    slope_up, param_up, param_down = arrays
    return (
        mesh.shape["replica"] == 2
        and mesh.shape["model"] > 1
        and param_up.shape[0] % LANES == 0
        and param_up.shape[0] > LANES
        and param_up.shape[1] == param_down.shape[0]
        and param_down.shape[1] == param_up.shape[0]
        and param_up.shape[1] % LANES == 0
        and param_down.shape[0] % LANES == 0
    )


def step(mesh, slope_up, slope_down, slope_norm, param_up, param_down, param_norm):
    args = (slope_up, slope_down, slope_norm, param_up, param_down, param_norm)
    if suits(mesh, slope_up, param_up, param_down):
        return fused(mesh.shape["replica"], mesh.shape["model"], *args)
    return shards(*args)


OUT = pltpu.VMEM


def solution(mesh):
    return jax.shard_map(
        functools.partial(step, mesh),
        mesh=mesh,
        in_specs=(
            P(("copy", "replica"), None, "model"),
            P(("copy", "replica"), "model", None),
            P(("copy", "replica"), None),
            P(("copy", "replica"), "model"),
            P(("copy", "model"), "replica"),
            P(("copy", "replica")),
        ),
        out_specs=(
            P("copy", "model"),
            P(("copy", "model"), None),
            P("copy"),
            P(("copy", "replica"), "model"),
            P(("copy", "model"), "replica"),
            P(("copy", "replica")),
        ),
        check_vma=False,
    )
```

```python
import functools

import jax
import jax.numpy as jnp
from jax import lax
from jax.experimental import pallas as pl
from jax.experimental.pallas import tpu as pltpu
from jax.sharding import PartitionSpec as P

learn_rate = 0.5


def shards(slope_up, slope_down, slope_norm, param_up, param_down, param_norm):
    mean_up, mean_down = (
        lax.psum_scatter(
            slope_up[0].astype(jnp.float32).astype(jnp.bfloat16),
            "replica",
            scatter_dimension=0,
            tiled=True,
        ).astype(jnp.float32),
        lax.psum_scatter(
            slope_down[0].astype(jnp.float32).astype(jnp.bfloat16),
            "replica",
            scatter_dimension=1,
            tiled=True,
        ).astype(jnp.float32),
    )
    whole_norm = lax.psum(slope_norm[0].astype(jnp.float32), "replica")
    place = lax.axis_index("replica")
    mean_norm = lax.dynamic_slice_in_dim(
        whole_norm, place * param_norm.shape[0], param_norm.shape[0]
    )
    mean_rate = lax.axis_size("replica") ** (-0.5)
    mean_up = mean_up * mean_rate
    mean_down = mean_down * mean_rate
    mean_norm = mean_norm * mean_rate
    own_up, own_down, slope_up_norm, slope_down_norm = lax.psum(
        (
            jnp.sum(param_up * param_up, axis=1, keepdims=True),
            jnp.sum(param_down * param_down, axis=0, keepdims=True),
            jnp.sum(mean_up * mean_up, axis=1, keepdims=True),
            jnp.sum(mean_down * mean_down, axis=0, keepdims=True),
        ),
        "model",
    )
    mean_up = mean_up * (jnp.sqrt(own_up) * lax.rsqrt(slope_up_norm + 1e-06))
    mean_down = mean_down * (jnp.sqrt(own_down) * lax.rsqrt(slope_down_norm + 1e-06))
    next_up = param_up - learn_rate * mean_up
    next_down = param_down - learn_rate * mean_down
    next_norm = param_norm - learn_rate * mean_norm
    half_up, half_down, half_norm = (
        lax.all_gather(next_up.astype(jnp.bfloat16), "replica", axis=0, tiled=True),
        lax.all_gather(next_down.astype(jnp.bfloat16), "replica", axis=1, tiled=True),
        lax.all_gather(next_norm.astype(jnp.bfloat16), "replica", axis=0, tiled=True),
    )
    return (half_up, half_down, half_norm, next_up, next_down, next_norm)


MESH = pl.DeviceIdType.MESH
LANES = 128
ROWS = 32
AHEAD = 9
DOWN_CUTS = 4


def update_kernel(
    replicas,
    models,
    slope_up,
    slope_down,
    slope_norm,
    param_up,
    param_down,
    param_norm,
    half_up,
    half_down,
    half_norm,
    next_up,
    next_down,
    next_norm,
    own_up,
    peer_up,
    own_down,
    peer_down,
    own_vec,
    peer_vec,
    own_gain,
    peer_gain,
    sum_vec,
    gain,
    lent_param,
    lent_slope,
    lent_own,
    lent_norm,
    piece,
    got_piece,
    square,
    spread,
    load_sem,
    send_sem,
    slope_recv,
    half_recv,
    piece_recv,
    lent_recv,
    pair_ready,
    model_ready,
):
    me = lax.axis_index("replica")
    other = 1 - me
    spot = lax.axis_index("model")
    share, inner = param_up.shape
    depth = param_down.shape[0]
    down_per, down_rows = steps_of(depth)
    mine = pl.multiple_of(me * share, LANES)
    theirs = pl.multiple_of(other * share, LANES)
    rate = replicas ** (-0.5)
    f32 = jnp.float32
    pieces = pieces_of(share)

    loads = {}

    def load(name, source, target):
        copy = pltpu.make_async_copy(source, target, load_sem.at[len(loads)])
        copy.start()
        loads[name] = copy

    def pair_copy(source, target, send, recv):
        return pltpu.make_async_remote_copy(
            source,
            target,
            send_sem.at[send],
            recv,
            device_id={"replica": other},
            device_id_type=MESH,
        )

    def own_slope(kind, start, size):
        if kind == "up":
            return slope_up.at[0, pl.ds(mine + start, size), :]
        return slope_down.at[0, :, pl.ds(mine + start, size)]

    def peer_slope(kind, start, size):
        if kind == "up":
            return slope_up.at[0, pl.ds(theirs + start, size), :]
        return slope_down.at[0, :, pl.ds(theirs + start, size)]

    def cut(kind, up, down, start, size):
        if kind == "up":
            return up.at[pl.ds(start, size), :]
        return down.at[:, pl.ds(start, size)]

    barrier = pltpu.get_barrier_semaphore()
    lead = me == replicas - 1

    @pl.when(lead)
    def _():
        pl.semaphore_signal(
            barrier, inc=1, device_id={"replica": other}, device_id_type=MESH
        )

    @pl.when(jnp.logical_not(lead))
    def _():
        pl.semaphore_wait(barrier, 1)
        pl.semaphore_signal(
            pair_ready, inc=1, device_id={"replica": other}, device_id_type=MESH
        )

    spare = share - LANES
    first = {}
    parts = [("down", 0, LANES), ("down", LANES, share - LANES), ("up", 0, share)]
    for span in parts:
        if span[2]:
            load(
                ("param", span),
                cut(span[0], param_up, param_down, *span[1:]),
                cut(span[0], next_up, next_down, *span[1:]),
            )
            load(
                ("slope", span),
                own_slope(*span),
                cut(span[0], own_up, own_down, *span[1:]),
            )
            for piece_span in pieces:
                if piece_span[0] == span[0] and piece_span[1] == span[1]:
                    first[piece_span] = span
    load("slope norm", slope_norm, own_vec)
    load("param norm", param_norm, own_gain)

    @pl.when(jnp.logical_and(spot == 0, lead))
    def _():
        pltpu.make_async_copy(
            peer_slope("up", spare, LANES), lent_own, load_sem.at[8]
        ).start()

    @pl.when(lead)
    def _():
        pl.semaphore_wait(pair_ready, 1)
        for k in range(1, models):
            pl.semaphore_signal(
                barrier,
                inc=1,
                device_id={"model": lax.rem(spot + k, models)},
                device_id_type=MESH,
            )

    def meet_models():
        @pl.when(lead)
        def _():
            pl.semaphore_wait(barrier, models - 1)
            pl.semaphore_signal(
                model_ready, inc=1, device_id={"replica": other}, device_id_type=MESH
            )

        @pl.when(jnp.logical_not(lead))
        def _():
            pl.semaphore_wait(model_ready, 1)

    for n, span in enumerate(pieces):
        pair_copy(
            peer_slope(*span),
            cut(span[0], peer_up, peer_down, *span[1:]),
            0,
            slope_recv.at[n],
        ).start()
    norms = [
        pair_copy(slope_norm, peer_vec, 1, slope_recv.at[len(pieces)]),
        pair_copy(param_norm, peer_gain, 2, slope_recv.at[len(pieces) + 1]),
    ]
    for copy in norms:
        copy.start()

    last = len(pieces) - 1
    gives = jnp.logical_and(spot == 0, jnp.logical_not(lead))
    takes = jnp.logical_and(spot == 0, lead)
    lent = (
        pair_copy(param_up.at[pl.ds(spare, LANES), :], lent_param, 6, lent_recv.at[0]),
        pair_copy(own_slope("up", spare, LANES), lent_slope, 6, lent_recv.at[0]),
    )
    both = next_up.at[pl.ds(0, LANES + LANES // 2), :]
    lent_both = pair_copy(both, both, 6, lent_recv.at[0])

    @pl.when(gives)
    def _():
        for copy in lent:
            copy.start()

    def norm_copy(source, target, n, k):
        return pltpu.make_async_remote_copy(
            source,
            target,
            send_sem.at[4],
            piece_recv.at[n],
            device_id={"model": lax.rem(spot + k, models)},
            device_id_type=MESH,
        )

    def share_norm(n):
        for j in range(models - 1):
            k = lax.rem(jnp.where(j < spot, j, j + 1) - spot + models, models)
            norm_copy(piece.at[n], got_piece.at[n, k - 1], n, k).start()

    def lend_norm(source, target):
        return pltpu.make_async_remote_copy(
            source,
            target,
            send_sem.at[5],
            lent_recv.at[1],
            device_id={"model": 0, "replica": other},
            device_id_type=MESH,
        )

    def whole_norm(n):
        norm_copy(got_piece.at[n], got_piece.at[n], n, 1).wait_recv()
        total = piece[n]
        for k in range(1, models):
            total = total + got_piece[n, k - 1]
        return total

    def ratio_of(whole):
        return jnp.sqrt(whole[0:1]) * (rate * learn_rate) * lax.rsqrt(
            whole[1:2] * (rate * rate) + 1e-06
        )

    square[...] = jnp.zeros(square.shape, f32)

    def row_squares(start, size, value):
        for r in range(size // ROWS):
            rows = pl.ds(start + r * ROWS, ROWS)
            total = jnp.zeros((ROWS, LANES), f32)
            for j in range(inner // LANES):
                x = value(rows, pl.ds(j * LANES, LANES))
                total = total + x * x
            square[pl.ds(r * ROWS, ROWS), :] = total

        return jnp.sum(square[...].T, axis=0, keepdims=True)

    def column_squares(start, size, value):
        def body(r, total):
            for q in range(down_rows // ROWS):
                x = value(pl.ds(r * down_rows + q * ROWS, ROWS), pl.ds(start, size))
                total = total + x * x
            return total

        total = lax.fori_loop(
            0, depth // down_rows, body, jnp.zeros((ROWS, LANES), f32)
        )
        return jnp.sum(total, axis=0, keepdims=True)

    def sum_up(rows, lanes):
        return own_up[rows, lanes].astype(f32) + peer_up[rows, lanes].astype(f32)

    def sum_down(rows, lanes):
        return own_down[rows, lanes].astype(f32) + peer_down[rows, lanes].astype(f32)

    def measure_piece(n):
        kind, start, size = pieces[n]
        squares = row_squares if kind == "up" else column_squares
        param = next_up if kind == "up" else next_down
        total = sum_up if kind == "up" else sum_down
        span = first.get(pieces[n])
        if span:
            loads["param", span].wait()
        piece[n, 0:1] = squares(start, size, lambda rows, lanes: param[rows, lanes])
        if span:
            loads["slope", span].wait()
        pair_copy(
            peer_slope(*pieces[n]),
            cut(kind, peer_up, peer_down, start, size),
            0,
            slope_recv.at[n],
        ).wait_recv()
        piece[n, 1:2] = squares(start, size, total)
        if n == 0:
            meet_models()
        share_norm(n)
        if n == last:

            @pl.when(jnp.logical_not(lead))
            def _():
                lend_norm(piece.at[n], lent_norm.at[models - 1 - spot]).start()

    def update_piece(n):
        kind, start, size = pieces[n]
        ratio = ratio_of(whole_norm(n))
        if kind == "up":
            update_up(start, size, ratio)
        else:
            update_down(start, size, ratio)

    def update_up(start, size, ratio):
        spread[...] = jnp.broadcast_to(ratio, (LANES, LANES)).T

        @pl.loop(0, size // ROWS)
        def _(r):
            rows = pl.ds(start + r * ROWS, ROWS)
            scale = spread[pl.ds(r * ROWS, ROWS), :]
            for j in range(inner // LANES):
                lanes = pl.ds(j * LANES, LANES)
                new = next_up[rows, lanes] - sum_up(rows, lanes) * scale
                next_up[rows, lanes] = new
                half_up[pl.ds(mine + start + r * ROWS, ROWS), lanes] = new.astype(
                    jnp.bfloat16
                )

        def push_half():
            block = half_up.at[pl.ds(mine + start, size), :]
            pair_copy(block, block, 3, half_recv.at[0]).start()

        if start == spare:
            pl.when(jnp.logical_not(gives))(push_half)
        else:
            push_half()

    def update_down(start, size, ratio):
        scale = jnp.broadcast_to(ratio, (ROWS, LANES))
        lanes = pl.ds(start, size)
        place = pl.ds(mine + start, size)

        per = down_per

        @pl.loop(0, depth // per)
        def _(p):
            @pl.loop(0, per // down_rows)
            def _(r):
                for q in range(down_rows // ROWS):
                    rows = pl.ds(p * per + r * down_rows + q * ROWS, ROWS)
                    new = next_down[rows, lanes] - sum_down(rows, lanes) * scale
                    next_down[rows, lanes] = new
                    half_down[rows, place] = new.astype(jnp.bfloat16)

            block = half_down.at[pl.ds(p * per, per), place]
            pair_copy(block, block, 3, half_recv.at[0]).start()

    def update_norm():
        loads["slope norm"].wait()
        loads["param norm"].wait()
        for copy in norms:
            copy.wait_recv()
        sum_vec[...] = (
            (own_vec[...].astype(f32) + peer_vec[...].astype(f32)) * rate * learn_rate
        )
        new_gain = own_gain[...].reshape(1, share) - sum_vec[:, pl.ds(mine, share)]
        gain[:, pl.ds(mine, share)] = new_gain
        gain[:, pl.ds(theirs, share)] = (
            peer_gain[...].reshape(1, share) - sum_vec[:, pl.ds(theirs, share)]
        )
        next_norm[...] = new_gain.reshape(share)
        half_norm[...] = gain[...].reshape(half_norm.shape).astype(jnp.bfloat16)

    ahead = min(AHEAD, len(pieces))
    for n in range(len(pieces) + ahead):
        if n < len(pieces):
            measure_piece(n)
        if n == ahead + 2:
            update_norm()
        if n >= ahead:
            update_piece(n - ahead)
    @pl.when(takes)
    def _():
        lent_both.wait_recv()
        pltpu.make_async_copy(
            peer_slope("up", spare, LANES), lent_own, load_sem.at[8]
        ).wait()
        lend_norm(lent_norm, lent_norm).wait_recv()
        whole = lent_norm[models - 1]
        for k in range(1, models):
            whole = whole + lent_norm[k - 1]
        spread[...] = jnp.broadcast_to(ratio_of(whole), (LANES, LANES)).T

        @pl.loop(0, LANES // ROWS)
        def _(r):
            rows = pl.ds(r * ROWS, ROWS)
            scale = spread[rows, :]
            for j in range(inner // LANES):
                lanes = pl.ds(j * LANES, LANES)
                total = lent_slope[rows, lanes].astype(f32) + lent_own[
                    rows, lanes
                ].astype(f32)
                half_up[pl.ds(theirs + spare + r * ROWS, ROWS), lanes] = (
                    lent_param[rows, lanes] - total * scale
                ).astype(jnp.bfloat16)

    pair_copy(half_up, half_up, 0, half_recv.at[0]).wait_send()

    def halves(rows):
        block = half_up.at[pl.ds(0, rows), :]
        return pair_copy(block, block, 3, half_recv.at[0])

    @pl.when(gives)
    def _():
        halves(2 * share - LANES).wait_send()
        lent_both.wait_send()

    @pl.when(jnp.logical_not(gives))
    def _():
        halves(2 * share).wait_send()

    @pl.when(takes)
    def _():
        halves(2 * share - LANES).wait_recv()

    @pl.when(jnp.logical_not(takes))
    def _():
        halves(2 * share).wait_recv()

    @pl.when(jnp.logical_not(lead))
    def _():
        lend_norm(piece.at[last], lent_norm.at[0]).wait_send()

    for copy in norms:
        copy.wait_send()
    norm_copy(got_piece, got_piece, 0, 1).wait_send()


def steps_of(depth):
    cuts = max(c for c in range(1, DOWN_CUTS + 1) if depth % (c * ROWS) == 0)
    per = depth // cuts
    return per, max(k * ROWS for k in range(1, 11) if per % (k * ROWS) == 0)


def pieces_of(share):
    pieces = [("down", start, LANES) for start in range(0, share, LANES)]
    pieces += [("up", start, LANES) for start in range(0, share, LANES)]
    return pieces


def write_kernel(
    half_up,
    half_down,
    half_norm,
    next_up,
    next_down,
    next_norm,
    half_up_out,
    half_down_out,
    half_norm_out,
    next_up_out,
    next_down_out,
    next_norm_out,
    sem,
):
    moves = (
        (half_norm, half_norm_out),
        (next_norm, next_norm_out),
        (half_up, half_up_out),
        (half_down, half_down_out),
        (next_up, next_up_out),
        (next_down, next_down_out),
    )
    for i, (source, target) in enumerate(moves):
        cuts = 8 if len(source.shape) == 2 else 1
        rows = source.shape[0] // cuts
        for c in range(cuts):
            part = pl.ds(c * rows, rows)
            pltpu.make_async_copy(source.at[part], target.at[part], sem.at[i]).start()
    for i, (source, target) in enumerate(moves):
        pltpu.make_async_copy(source, target, sem.at[i]).wait()


def fused(replicas, models, slope_up, slope_down, slope_norm, param_up, param_down, param_norm):
    share, inner = param_up.shape
    depth = param_down.shape[0]
    width = slope_up.shape[1]
    count = len(pieces_of(share))
    bf16, f32 = jnp.bfloat16, jnp.float32
    hbm = pl.BlockSpec(memory_space=pltpu.HBM)
    vmem = pl.BlockSpec(memory_space=pltpu.VMEM)
    outs = pl.pallas_call(
        functools.partial(update_kernel, replicas, models),
        out_shape=(
            OUT((width, inner), bf16),
            OUT((depth, width), bf16),
            OUT((width,), bf16),
            OUT((share, inner), f32),
            OUT((depth, share), f32),
            OUT((share,), f32),
        ),
        in_specs=[hbm] * 6,
        out_specs=(vmem,) * 6,
        scratch_shapes=[
            pltpu.VMEM((share, inner), bf16),
            pltpu.VMEM((share, inner), bf16),
            pltpu.VMEM((depth, share), bf16),
            pltpu.VMEM((depth, share), bf16),
            pltpu.VMEM((1, width), bf16),
            pltpu.VMEM((1, width), bf16),
            pltpu.VMEM((share,), f32),
            pltpu.VMEM((share,), f32),
            pltpu.VMEM((1, width), f32),
            pltpu.VMEM((1, width), f32),
            pltpu.VMEM((LANES, inner), f32),
            pltpu.VMEM((LANES, inner), bf16),
            pltpu.VMEM((LANES, inner), bf16),
            pltpu.VMEM((models, 2, LANES), f32),
            pltpu.VMEM((count, 2, LANES), f32),
            pltpu.VMEM((count, models - 1, 2, LANES), f32),
            pltpu.VMEM((LANES, LANES), f32),
            pltpu.VMEM((LANES, LANES), f32),
            pltpu.SemaphoreType.DMA((9,)),
            pltpu.SemaphoreType.DMA((7,)),
            pltpu.SemaphoreType.DMA((count + 2,)),
            pltpu.SemaphoreType.DMA((1,)),
            pltpu.SemaphoreType.DMA((count,)),
            pltpu.SemaphoreType.DMA((2,)),
            pltpu.SemaphoreType.REGULAR,
            pltpu.SemaphoreType.REGULAR,
        ],
        compiler_params=pltpu.CompilerParams(
            collective_id=0, has_side_effects=True, vmem_limit_bytes=24 * 2**20
        ),
    )(
        *(
            pltpu.with_memory_space_constraint(x, pltpu.HBM)
            for x in (
                slope_up, slope_down, slope_norm, param_up, param_down, param_norm
            )
        )
    )
    return pl.pallas_call(
        write_kernel,
        out_shape=(
            jax.ShapeDtypeStruct((width, inner), bf16),
            jax.ShapeDtypeStruct((depth, width), bf16),
            jax.ShapeDtypeStruct((width,), bf16),
            jax.ShapeDtypeStruct((share, inner), f32),
            jax.ShapeDtypeStruct((depth, share), f32),
            jax.ShapeDtypeStruct((share,), f32),
        ),
        in_specs=[vmem] * 6,
        out_specs=(hbm,) * 6,
        scratch_shapes=[pltpu.SemaphoreType.DMA((6,))],
        compiler_params=pltpu.CompilerParams(vmem_limit_bytes=24 * 2**20),
    )(*(pltpu.with_memory_space_constraint(x, pltpu.VMEM) for x in outs))


def suits(mesh, *arrays):
    slope_up, param_up, param_down = arrays
    return (
        mesh.shape["replica"] == 2
        and mesh.shape["model"] > 1
        and param_up.shape[0] % LANES == 0
        and param_up.shape[0] > LANES
        and param_up.shape[1] == param_down.shape[0]
        and param_down.shape[1] == param_up.shape[0]
        and param_up.shape[1] % LANES == 0
        and param_down.shape[0] % LANES == 0
    )


def step(mesh, slope_up, slope_down, slope_norm, param_up, param_down, param_norm):
    args = (slope_up, slope_down, slope_norm, param_up, param_down, param_norm)
    if suits(mesh, slope_up, param_up, param_down):
        return fused(mesh.shape["replica"], mesh.shape["model"], *args)
    return shards(*args)


OUT = pltpu.VMEM


def solution(mesh):
    return jax.shard_map(
        functools.partial(step, mesh),
        mesh=mesh,
        in_specs=(
            P(("copy", "replica"), None, "model"),
            P(("copy", "replica"), "model", None),
            P(("copy", "replica"), None),
            P(("copy", "replica"), "model"),
            P(("copy", "model"), "replica"),
            P(("copy", "replica")),
        ),
        out_specs=(
            P("copy", "model"),
            P(("copy", "model"), None),
            P("copy"),
            P(("copy", "replica"), "model"),
            P(("copy", "model"), "replica"),
            P(("copy", "replica")),
        ),
        check_vma=False,
    )
```

```python
import functools

import jax
import jax.numpy as jnp
from jax import lax
from jax.experimental import pallas as pl
from jax.experimental.pallas import tpu as pltpu
from jax.sharding import PartitionSpec as P

learn_rate = 0.5


def shards(slope_up, slope_down, slope_norm, param_up, param_down, param_norm):
    mean_up, mean_down = (
        lax.psum_scatter(
            slope_up[0].astype(jnp.float32).astype(jnp.bfloat16),
            "replica",
            scatter_dimension=0,
            tiled=True,
        ).astype(jnp.float32),
        lax.psum_scatter(
            slope_down[0].astype(jnp.float32).astype(jnp.bfloat16),
            "replica",
            scatter_dimension=1,
            tiled=True,
        ).astype(jnp.float32),
    )
    whole_norm = lax.psum(slope_norm[0].astype(jnp.float32), "replica")
    place = lax.axis_index("replica")
    mean_norm = lax.dynamic_slice_in_dim(
        whole_norm, place * param_norm.shape[0], param_norm.shape[0]
    )
    mean_rate = lax.axis_size("replica") ** (-0.5)
    mean_up = mean_up * mean_rate
    mean_down = mean_down * mean_rate
    mean_norm = mean_norm * mean_rate
    own_up, own_down, slope_up_norm, slope_down_norm = lax.psum(
        (
            jnp.sum(param_up * param_up, axis=1, keepdims=True),
            jnp.sum(param_down * param_down, axis=0, keepdims=True),
            jnp.sum(mean_up * mean_up, axis=1, keepdims=True),
            jnp.sum(mean_down * mean_down, axis=0, keepdims=True),
        ),
        "model",
    )
    mean_up = mean_up * (jnp.sqrt(own_up) * lax.rsqrt(slope_up_norm + 1e-06))
    mean_down = mean_down * (jnp.sqrt(own_down) * lax.rsqrt(slope_down_norm + 1e-06))
    next_up = param_up - learn_rate * mean_up
    next_down = param_down - learn_rate * mean_down
    next_norm = param_norm - learn_rate * mean_norm
    half_up, half_down, half_norm = (
        lax.all_gather(next_up.astype(jnp.bfloat16), "replica", axis=0, tiled=True),
        lax.all_gather(next_down.astype(jnp.bfloat16), "replica", axis=1, tiled=True),
        lax.all_gather(next_norm.astype(jnp.bfloat16), "replica", axis=0, tiled=True),
    )
    return (half_up, half_down, half_norm, next_up, next_down, next_norm)


MESH = pl.DeviceIdType.MESH
LANES = 128
ROWS = 32
DOWN_CUTS = 4


def update_kernel(
    replicas,
    models,
    slope_up,
    slope_down,
    slope_norm,
    param_up,
    param_down,
    param_norm,
    half_up,
    half_down,
    half_norm,
    next_up,
    next_down,
    next_norm,
    own_up,
    peer_up,
    own_down,
    peer_down,
    own_vec,
    peer_vec,
    own_gain,
    peer_gain,
    sum_vec,
    gain,
    lent_param,
    lent_slope,
    lent_own,
    lent_norm,
    piece,
    got_piece,
    square,
    spread,
    lent_load,
    send_sem,
    half_recv,
    piece_recv,
    lent_recv,
    pair_ready,
    model_ready,
):
    me = lax.axis_index("replica")
    other = 1 - me
    spot = lax.axis_index("model")
    share, inner = param_up.shape
    depth = param_down.shape[0]
    down_per, down_rows = steps_of(depth)
    mine = pl.multiple_of(me * share, LANES)
    theirs = pl.multiple_of(other * share, LANES)
    rate = replicas ** (-0.5)
    f32 = jnp.float32
    pieces = pieces_of(share)

    def pair_copy(source, target, send, recv):
        return pltpu.make_async_remote_copy(
            source,
            target,
            send,
            recv,
            device_id={"replica": other},
            device_id_type=MESH,
        )

    def own_slope(kind, start, size):
        if kind == "up":
            return slope_up.at[0, pl.ds(mine + start, size), :]
        return slope_down.at[0, :, pl.ds(mine + start, size)]

    def peer_slope(kind, start, size):
        if kind == "up":
            return slope_up.at[0, pl.ds(theirs + start, size), :]
        return slope_down.at[0, :, pl.ds(theirs + start, size)]

    def cut(kind, up, down, start, size):
        if kind == "up":
            return up.at[pl.ds(start, size), :]
        return down.at[:, pl.ds(start, size)]

    lead = me == replicas - 1
    spare = share - LANES
    last = len(pieces) - 1
    gives = jnp.logical_and(spot == 0, jnp.logical_not(lead))
    takes = jnp.logical_and(spot == 0, lead)
    lent = (
        pair_copy(param_up.at[pl.ds(spare, LANES), :], lent_param, send_sem.at[3], lent_recv.at[0]),
        pair_copy(own_slope("up", spare, LANES), lent_slope, send_sem.at[3], lent_recv.at[0]),
    )
    both = next_up.at[pl.ds(0, LANES + LANES // 2), :]
    lent_both = pair_copy(both, both, send_sem.at[3], lent_recv.at[0])

    def norm_copy(source, target, n, k):
        return pltpu.make_async_remote_copy(
            source,
            target,
            send_sem.at[1],
            piece_recv.at[n],
            device_id={"model": lax.rem(spot + k, models)},
            device_id_type=MESH,
        )

    def share_norm(n):
        for j in range(models - 1):
            k = lax.rem(jnp.where(j < spot, j, j + 1) - spot + models, models)
            norm_copy(piece.at[n], got_piece.at[n, k - 1], n, k).start()

    def lend_norm(source, target):
        return pltpu.make_async_remote_copy(
            source,
            target,
            send_sem.at[2],
            lent_recv.at[1],
            device_id={"model": 0, "replica": other},
            device_id_type=MESH,
        )

    def whole_norm(n):
        norm_copy(got_piece.at[n], got_piece.at[n], n, 1).wait_recv()
        total = piece[n]
        for k in range(1, models):
            total = total + got_piece[n, k - 1]
        return total

    def ratio_of(whole):
        return jnp.sqrt(whole[0:1]) * (rate * learn_rate) * lax.rsqrt(
            whole[1:2] * (rate * rate) + 1e-06
        )

    square[...] = jnp.zeros(square.shape, f32)

    def row_squares(start, size, value):
        for r in range(size // ROWS):
            rows = pl.ds(start + r * ROWS, ROWS)
            total = jnp.zeros((ROWS, LANES), f32)
            for j in range(inner // LANES):
                x = value(rows, pl.ds(j * LANES, LANES))
                total = total + x * x
            square[pl.ds(r * ROWS, ROWS), :] = total

        return jnp.sum(square[...].T, axis=0, keepdims=True)

    def column_squares(start, size, value):
        def body(r, total):
            for q in range(down_rows // ROWS):
                x = value(pl.ds(r * down_rows + q * ROWS, ROWS), pl.ds(start, size))
                total = total + x * x
            return total

        total = lax.fori_loop(
            0, depth // down_rows, body, jnp.zeros((ROWS, LANES), f32)
        )
        return jnp.sum(total, axis=0, keepdims=True)

    def sum_up(rows, lanes):
        return own_up[rows, lanes].astype(f32) + peer_up[rows, lanes].astype(f32)

    def sum_down(rows, lanes):
        return own_down[rows, lanes].astype(f32) + peer_down[rows, lanes].astype(f32)

    def update_piece(n):
        kind, start, size = pieces[n]
        ratio = ratio_of(whole_norm(n))
        if kind == "up":
            update_up(start, size, ratio)
        else:
            update_down(start, size, ratio)

    def update_up(start, size, ratio):
        spread[...] = jnp.broadcast_to(ratio, (LANES, LANES)).T

        @pl.loop(0, size // ROWS)
        def _(r):
            rows = pl.ds(start + r * ROWS, ROWS)
            scale = spread[pl.ds(r * ROWS, ROWS), :]
            for j in range(inner // LANES):
                lanes = pl.ds(j * LANES, LANES)
                new = next_up[rows, lanes] - sum_up(rows, lanes) * scale
                next_up[rows, lanes] = new
                half_up[pl.ds(mine + start + r * ROWS, ROWS), lanes] = new.astype(
                    jnp.bfloat16
                )

        def push_half():
            block = half_up.at[pl.ds(mine + start, size), :]
            pair_copy(block, block, send_sem.at[0], half_recv.at[0]).start()

        if start == spare:
            pl.when(jnp.logical_not(gives))(push_half)
        else:
            push_half()

    def update_down(start, size, ratio):
        scale = jnp.broadcast_to(ratio, (ROWS, LANES))
        lanes = pl.ds(start, size)
        place = pl.ds(mine + start, size)

        per = down_per

        @pl.loop(0, depth // per)
        def _(p):
            @pl.loop(0, per // down_rows)
            def _(r):
                for q in range(down_rows // ROWS):
                    rows = pl.ds(p * per + r * down_rows + q * ROWS, ROWS)
                    new = next_down[rows, lanes] - sum_down(rows, lanes) * scale
                    next_down[rows, lanes] = new
                    half_down[rows, place] = new.astype(jnp.bfloat16)

            block = half_down.at[pl.ds(p * per, per), place]
            pair_copy(block, block, send_sem.at[0], half_recv.at[0]).start()

    def exchange(load_sem, early_send, slope_recv):
        loads = {}

        def load(name, source, target):
            copy = pltpu.make_async_copy(source, target, load_sem.at[len(loads)])
            copy.start()
            loads[name] = copy

        barrier = pltpu.get_barrier_semaphore()

        @pl.when(lead)
        def _():
            pl.semaphore_signal(
                barrier, inc=1, device_id={"replica": other}, device_id_type=MESH
            )

        @pl.when(jnp.logical_not(lead))
        def _():
            pl.semaphore_wait(barrier, 1)
            pl.semaphore_signal(
                pair_ready, inc=1, device_id={"replica": other}, device_id_type=MESH
            )

        first = {}
        parts = [("down", 0, LANES), ("down", LANES, share - LANES), ("up", 0, share)]
        for span in parts:
            if span[2]:
                load(
                    ("param", span),
                    cut(span[0], param_up, param_down, *span[1:]),
                    cut(span[0], next_up, next_down, *span[1:]),
                )
                load(
                    ("slope", span),
                    own_slope(*span),
                    cut(span[0], own_up, own_down, *span[1:]),
                )
                for piece_span in pieces:
                    if piece_span[0] == span[0] and piece_span[1] == span[1]:
                        first[piece_span] = span
        load("slope norm", slope_norm, own_vec)
        load("param norm", param_norm, own_gain)

        @pl.when(jnp.logical_and(spot == 0, lead))
        def _():
            pltpu.make_async_copy(
                peer_slope("up", spare, LANES), lent_own, lent_load.at[0]
            ).start()

        @pl.when(lead)
        def _():
            pl.semaphore_wait(pair_ready, 1)
            for k in range(1, models):
                pl.semaphore_signal(
                    barrier,
                    inc=1,
                    device_id={"model": lax.rem(spot + k, models)},
                    device_id_type=MESH,
                )

        def meet_models():
            @pl.when(lead)
            def _():
                pl.semaphore_wait(barrier, models - 1)
                pl.semaphore_signal(
                    model_ready, inc=1, device_id={"replica": other}, device_id_type=MESH
                )

            @pl.when(jnp.logical_not(lead))
            def _():
                pl.semaphore_wait(model_ready, 1)

        for n, span in enumerate(pieces):
            pair_copy(
                peer_slope(*span),
                cut(span[0], peer_up, peer_down, *span[1:]),
                early_send.at[0],
                slope_recv.at[n],
            ).start()
        norms = [
            pair_copy(slope_norm, peer_vec, early_send.at[1], slope_recv.at[len(pieces)]),
            pair_copy(param_norm, peer_gain, early_send.at[2], slope_recv.at[len(pieces) + 1]),
        ]
        for copy in norms:
            copy.start()

        @pl.when(gives)
        def _():
            for copy in lent:
                copy.start()

        def measure_piece(n):
            kind, start, size = pieces[n]
            squares = row_squares if kind == "up" else column_squares
            param = next_up if kind == "up" else next_down
            total = sum_up if kind == "up" else sum_down
            span = first.get(pieces[n])
            if span:
                loads["param", span].wait()
            piece[n, 0:1] = squares(start, size, lambda rows, lanes: param[rows, lanes])
            if span:
                loads["slope", span].wait()
            pair_copy(
                peer_slope(*pieces[n]),
                cut(kind, peer_up, peer_down, start, size),
                early_send.at[0],
                slope_recv.at[n],
            ).wait_recv()
            piece[n, 1:2] = squares(start, size, total)
            if n == 0:
                meet_models()
            share_norm(n)
            if n == last:

                @pl.when(jnp.logical_not(lead))
                def _():
                    lend_norm(piece.at[n], lent_norm.at[models - 1 - spot]).start()

        def update_norm():
            loads["slope norm"].wait()
            loads["param norm"].wait()
            for copy in norms:
                copy.wait_recv()
            sum_vec[...] = (
                (own_vec[...].astype(f32) + peer_vec[...].astype(f32)) * rate * learn_rate
            )
            new_gain = own_gain[...].reshape(1, share) - sum_vec[:, pl.ds(mine, share)]
            gain[:, pl.ds(mine, share)] = new_gain
            gain[:, pl.ds(theirs, share)] = (
                peer_gain[...].reshape(1, share) - sum_vec[:, pl.ds(theirs, share)]
            )
            next_norm[...] = new_gain.reshape(share)
            half_norm[...] = gain[...].reshape(half_norm.shape).astype(jnp.bfloat16)

        for n in range(len(pieces)):
            measure_piece(n)
        update_norm()
        pair_copy(half_up, half_up, early_send.at[0], slope_recv.at[0]).wait_send()
        for copy in norms:
            copy.wait_send()

    pl.run_scoped(
        exchange,
        load_sem=pltpu.SemaphoreType.DMA((8,)),
        early_send=pltpu.SemaphoreType.DMA((3,)),
        slope_recv=pltpu.SemaphoreType.DMA((len(pieces) + 2,)),
    )
    for n in range(len(pieces)):
        update_piece(n)

    @pl.when(takes)
    def _():
        lent_both.wait_recv()
        pltpu.make_async_copy(
            peer_slope("up", spare, LANES), lent_own, lent_load.at[0]
        ).wait()
        lend_norm(lent_norm, lent_norm).wait_recv()
        whole = lent_norm[models - 1]
        for k in range(1, models):
            whole = whole + lent_norm[k - 1]
        spread[...] = jnp.broadcast_to(ratio_of(whole), (LANES, LANES)).T

        @pl.loop(0, LANES // ROWS)
        def _(r):
            rows = pl.ds(r * ROWS, ROWS)
            scale = spread[rows, :]
            for j in range(inner // LANES):
                lanes = pl.ds(j * LANES, LANES)
                total = lent_slope[rows, lanes].astype(f32) + lent_own[
                    rows, lanes
                ].astype(f32)
                half_up[pl.ds(theirs + spare + r * ROWS, ROWS), lanes] = (
                    lent_param[rows, lanes] - total * scale
                ).astype(jnp.bfloat16)

    def halves(rows):
        block = half_up.at[pl.ds(0, rows), :]
        return pair_copy(block, block, send_sem.at[0], half_recv.at[0])

    @pl.when(gives)
    def _():
        halves(2 * share - LANES).wait_send()
        lent_both.wait_send()

    @pl.when(jnp.logical_not(gives))
    def _():
        halves(2 * share).wait_send()

    @pl.when(takes)
    def _():
        halves(2 * share - LANES).wait_recv()

    @pl.when(jnp.logical_not(takes))
    def _():
        halves(2 * share).wait_recv()

    @pl.when(jnp.logical_not(lead))
    def _():
        lend_norm(piece.at[last], lent_norm.at[0]).wait_send()

    norm_copy(got_piece, got_piece, 0, 1).wait_send()


def steps_of(depth):
    cuts = max(c for c in range(1, DOWN_CUTS + 1) if depth % (c * ROWS) == 0)
    per = depth // cuts
    return per, max(k * ROWS for k in range(1, 11) if per % (k * ROWS) == 0)


def pieces_of(share):
    pieces = [("down", start, LANES) for start in range(0, share, LANES)]
    pieces += [("up", start, LANES) for start in range(0, share, LANES)]
    return pieces


def write_kernel(
    half_up,
    half_down,
    half_norm,
    next_up,
    next_down,
    next_norm,
    half_up_out,
    half_down_out,
    half_norm_out,
    next_up_out,
    next_down_out,
    next_norm_out,
    sem,
):
    moves = (
        (half_norm, half_norm_out),
        (next_norm, next_norm_out),
        (half_up, half_up_out),
        (half_down, half_down_out),
        (next_up, next_up_out),
        (next_down, next_down_out),
    )
    for i, (source, target) in enumerate(moves):
        cuts = 8 if len(source.shape) == 2 else 1
        rows = source.shape[0] // cuts
        for c in range(cuts):
            part = pl.ds(c * rows, rows)
            pltpu.make_async_copy(source.at[part], target.at[part], sem.at[i]).start()
    for i, (source, target) in enumerate(moves):
        pltpu.make_async_copy(source, target, sem.at[i]).wait()


def fused(replicas, models, slope_up, slope_down, slope_norm, param_up, param_down, param_norm):
    share, inner = param_up.shape
    depth = param_down.shape[0]
    width = slope_up.shape[1]
    count = len(pieces_of(share))
    bf16, f32 = jnp.bfloat16, jnp.float32
    hbm = pl.BlockSpec(memory_space=pltpu.HBM)
    vmem = pl.BlockSpec(memory_space=pltpu.VMEM)
    outs = pl.pallas_call(
        functools.partial(update_kernel, replicas, models),
        out_shape=(
            OUT((width, inner), bf16),
            OUT((depth, width), bf16),
            OUT((width,), bf16),
            OUT((share, inner), f32),
            OUT((depth, share), f32),
            OUT((share,), f32),
        ),
        in_specs=[hbm] * 6,
        out_specs=(vmem,) * 6,
        scratch_shapes=[
            pltpu.VMEM((share, inner), bf16),
            pltpu.VMEM((share, inner), bf16),
            pltpu.VMEM((depth, share), bf16),
            pltpu.VMEM((depth, share), bf16),
            pltpu.VMEM((1, width), bf16),
            pltpu.VMEM((1, width), bf16),
            pltpu.VMEM((share,), f32),
            pltpu.VMEM((share,), f32),
            pltpu.VMEM((1, width), f32),
            pltpu.VMEM((1, width), f32),
            pltpu.VMEM((LANES, inner), f32),
            pltpu.VMEM((LANES, inner), bf16),
            pltpu.VMEM((LANES, inner), bf16),
            pltpu.VMEM((models, 2, LANES), f32),
            pltpu.VMEM((count, 2, LANES), f32),
            pltpu.VMEM((count, models - 1, 2, LANES), f32),
            pltpu.VMEM((LANES, LANES), f32),
            pltpu.VMEM((LANES, LANES), f32),
            pltpu.SemaphoreType.DMA((1,)),
            pltpu.SemaphoreType.DMA((4,)),
            pltpu.SemaphoreType.DMA((1,)),
            pltpu.SemaphoreType.DMA((count,)),
            pltpu.SemaphoreType.DMA((2,)),
            pltpu.SemaphoreType.REGULAR,
            pltpu.SemaphoreType.REGULAR,
        ],
        compiler_params=pltpu.CompilerParams(
            collective_id=0, has_side_effects=True, vmem_limit_bytes=24 * 2**20
        ),
    )(
        *(
            pltpu.with_memory_space_constraint(x, pltpu.HBM)
            for x in (
                slope_up, slope_down, slope_norm, param_up, param_down, param_norm
            )
        )
    )
    return pl.pallas_call(
        write_kernel,
        out_shape=(
            jax.ShapeDtypeStruct((width, inner), bf16),
            jax.ShapeDtypeStruct((depth, width), bf16),
            jax.ShapeDtypeStruct((width,), bf16),
            jax.ShapeDtypeStruct((share, inner), f32),
            jax.ShapeDtypeStruct((depth, share), f32),
            jax.ShapeDtypeStruct((share,), f32),
        ),
        in_specs=[vmem] * 6,
        out_specs=(hbm,) * 6,
        scratch_shapes=[pltpu.SemaphoreType.DMA((6,))],
        compiler_params=pltpu.CompilerParams(vmem_limit_bytes=24 * 2**20),
    )(*(pltpu.with_memory_space_constraint(x, pltpu.VMEM) for x in outs))


def suits(mesh, *arrays):
    slope_up, param_up, param_down = arrays
    return (
        mesh.shape["replica"] == 2
        and mesh.shape["model"] > 1
        and param_up.shape[0] % LANES == 0
        and param_up.shape[0] > LANES
        and param_up.shape[1] == param_down.shape[0]
        and param_down.shape[1] == param_up.shape[0]
        and param_up.shape[1] % LANES == 0
        and param_down.shape[0] % LANES == 0
    )


def step(mesh, slope_up, slope_down, slope_norm, param_up, param_down, param_norm):
    args = (slope_up, slope_down, slope_norm, param_up, param_down, param_norm)
    if suits(mesh, slope_up, param_up, param_down):
        return fused(mesh.shape["replica"], mesh.shape["model"], *args)
    return shards(*args)


OUT = pltpu.VMEM


def solution(mesh):
    return jax.shard_map(
        functools.partial(step, mesh),
        mesh=mesh,
        in_specs=(
            P(("copy", "replica"), None, "model"),
            P(("copy", "replica"), "model", None),
            P(("copy", "replica"), None),
            P(("copy", "replica"), "model"),
            P(("copy", "model"), "replica"),
            P(("copy", "replica")),
        ),
        out_specs=(
            P("copy", "model"),
            P(("copy", "model"), None),
            P("copy"),
            P(("copy", "replica"), "model"),
            P(("copy", "model"), "replica"),
            P(("copy", "replica")),
        ),
        check_vma=False,
    )
```

```python
import functools

import jax
import jax.numpy as jnp
from jax import lax
from jax.experimental import pallas as pl
from jax.experimental.pallas import tpu as pltpu
from jax.sharding import PartitionSpec as P

learn_rate = 0.5


def shards(slope_up, slope_down, slope_norm, param_up, param_down, param_norm):
    mean_up, mean_down = (
        lax.psum_scatter(
            slope_up[0].astype(jnp.float32).astype(jnp.bfloat16),
            "replica",
            scatter_dimension=0,
            tiled=True,
        ).astype(jnp.float32),
        lax.psum_scatter(
            slope_down[0].astype(jnp.float32).astype(jnp.bfloat16),
            "replica",
            scatter_dimension=1,
            tiled=True,
        ).astype(jnp.float32),
    )
    whole_norm = lax.psum(slope_norm[0].astype(jnp.float32), "replica")
    place = lax.axis_index("replica")
    mean_norm = lax.dynamic_slice_in_dim(
        whole_norm, place * param_norm.shape[0], param_norm.shape[0]
    )
    mean_rate = lax.axis_size("replica") ** (-0.5)
    mean_up = mean_up * mean_rate
    mean_down = mean_down * mean_rate
    mean_norm = mean_norm * mean_rate
    own_up, own_down, slope_up_norm, slope_down_norm = lax.psum(
        (
            jnp.sum(param_up * param_up, axis=1, keepdims=True),
            jnp.sum(param_down * param_down, axis=0, keepdims=True),
            jnp.sum(mean_up * mean_up, axis=1, keepdims=True),
            jnp.sum(mean_down * mean_down, axis=0, keepdims=True),
        ),
        "model",
    )
    mean_up = mean_up * (jnp.sqrt(own_up) * lax.rsqrt(slope_up_norm + 1e-06))
    mean_down = mean_down * (jnp.sqrt(own_down) * lax.rsqrt(slope_down_norm + 1e-06))
    next_up = param_up - learn_rate * mean_up
    next_down = param_down - learn_rate * mean_down
    next_norm = param_norm - learn_rate * mean_norm
    half_up, half_down, half_norm = (
        lax.all_gather(next_up.astype(jnp.bfloat16), "replica", axis=0, tiled=True),
        lax.all_gather(next_down.astype(jnp.bfloat16), "replica", axis=1, tiled=True),
        lax.all_gather(next_norm.astype(jnp.bfloat16), "replica", axis=0, tiled=True),
    )
    return (half_up, half_down, half_norm, next_up, next_down, next_norm)


MESH = pl.DeviceIdType.MESH
LANES = 128
ROWS = 32
DOWN_CUTS = 4


def update_kernel(
    replicas,
    models,
    slope_up,
    slope_down,
    slope_norm,
    param_up,
    param_down,
    param_norm,
    half_up,
    half_down,
    half_norm,
    next_up,
    next_down,
    next_norm,
    own_up,
    peer_up,
    own_down,
    peer_down,
    own_vec,
    peer_vec,
    own_gain,
    peer_gain,
    sum_vec,
    gain,
    lent_param,
    lent_slope,
    lent_own,
    lent_norm,
    piece,
    got_piece,
    square,
    spread,
    lent_load,
    send_sem,
    half_recv,
    piece_recv,
    lent_recv,
    pair_ready,
    model_ready,
):
    me = lax.axis_index("replica")
    other = 1 - me
    spot = lax.axis_index("model")
    share, inner = param_up.shape
    depth = param_down.shape[0]
    down_per, down_rows = steps_of(depth)
    mine = pl.multiple_of(me * share, LANES)
    theirs = pl.multiple_of(other * share, LANES)
    rate = replicas ** (-0.5)
    f32 = jnp.float32
    pieces = pieces_of(share)

    def pair_copy(source, target, send, recv):
        return pltpu.make_async_remote_copy(
            source,
            target,
            send,
            recv,
            device_id={"replica": other},
            device_id_type=MESH,
        )

    def own_slope(kind, start, size):
        if kind == "up":
            return slope_up.at[0, pl.ds(mine + start, size), :]
        return slope_down.at[0, :, pl.ds(mine + start, size)]

    def peer_slope(kind, start, size):
        if kind == "up":
            return slope_up.at[0, pl.ds(theirs + start, size), :]
        return slope_down.at[0, :, pl.ds(theirs + start, size)]

    def cut(kind, up, down, start, size):
        if kind == "up":
            return up.at[pl.ds(start, size), :]
        return down.at[:, pl.ds(start, size)]

    lead = me == replicas - 1
    spare = share - LANES
    last = len(pieces) - 1
    gives = jnp.logical_and(spot == 0, jnp.logical_not(lead))
    takes = jnp.logical_and(spot == 0, lead)
    lent = (
        pair_copy(param_up.at[pl.ds(spare, LANES), :], lent_param, send_sem.at[3], lent_recv.at[0]),
        pair_copy(own_slope("up", spare, LANES), lent_slope, send_sem.at[3], lent_recv.at[0]),
    )
    both = next_up.at[pl.ds(0, LANES + LANES // 2), :]
    lent_both = pair_copy(both, both, send_sem.at[3], lent_recv.at[0])

    front = len(pieces) - 3
    scoped = []

    def norm_recv(n):
        if scoped and n < front:
            return scoped[0].at[n]
        return piece_recv.at[max(n - front, 0)]

    def norm_copy(source, target, n, k):
        return pltpu.make_async_remote_copy(
            source,
            target,
            send_sem.at[1],
            norm_recv(n),
            device_id={"model": lax.rem(spot + k, models)},
            device_id_type=MESH,
        )

    def share_norm(n):
        for j in range(models - 1):
            k = lax.rem(jnp.where(j < spot, j, j + 1) - spot + models, models)
            norm_copy(piece.at[n], got_piece.at[n, k - 1], n, k).start()

    def lend_norm(source, target):
        return pltpu.make_async_remote_copy(
            source,
            target,
            send_sem.at[2],
            lent_recv.at[1],
            device_id={"model": 0, "replica": other},
            device_id_type=MESH,
        )

    def whole_norm(n):
        norm_copy(got_piece.at[n], got_piece.at[n], n, 1).wait_recv()
        total = piece[n]
        for k in range(1, models):
            total = total + got_piece[n, k - 1]
        return total

    def ratio_of(whole):
        return jnp.sqrt(whole[0:1]) * (rate * learn_rate) * lax.rsqrt(
            whole[1:2] * (rate * rate) + 1e-06
        )

    square[...] = jnp.zeros(square.shape, f32)

    def row_squares(start, size, value):
        for r in range(size // ROWS):
            rows = pl.ds(start + r * ROWS, ROWS)
            total = jnp.zeros((ROWS, LANES), f32)
            for j in range(inner // LANES):
                x = value(rows, pl.ds(j * LANES, LANES))
                total = total + x * x
            square[pl.ds(r * ROWS, ROWS), :] = total

        return jnp.sum(square[...].T, axis=0, keepdims=True)

    def column_squares(start, size, value):
        def body(r, total):
            for q in range(down_rows // ROWS):
                x = value(pl.ds(r * down_rows + q * ROWS, ROWS), pl.ds(start, size))
                total = total + x * x
            return total

        total = lax.fori_loop(
            0, depth // down_rows, body, jnp.zeros((ROWS, LANES), f32)
        )
        return jnp.sum(total, axis=0, keepdims=True)

    def sum_up(rows, lanes):
        return own_up[rows, lanes].astype(f32) + peer_up[rows, lanes].astype(f32)

    def sum_down(rows, lanes):
        return own_down[rows, lanes].astype(f32) + peer_down[rows, lanes].astype(f32)

    def update_piece(n):
        kind, start, size = pieces[n]
        ratio = ratio_of(whole_norm(n))
        if kind == "up":
            update_up(start, size, ratio)
        else:
            update_down(start, size, ratio)

    def update_up(start, size, ratio):
        spread[...] = jnp.broadcast_to(ratio, (LANES, LANES)).T

        @pl.loop(0, size // ROWS)
        def _(r):
            rows = pl.ds(start + r * ROWS, ROWS)
            scale = spread[pl.ds(r * ROWS, ROWS), :]
            for j in range(inner // LANES):
                lanes = pl.ds(j * LANES, LANES)
                new = next_up[rows, lanes] - sum_up(rows, lanes) * scale
                next_up[rows, lanes] = new
                half_up[pl.ds(mine + start + r * ROWS, ROWS), lanes] = new.astype(
                    jnp.bfloat16
                )

        def push_half():
            block = half_up.at[pl.ds(mine + start, size), :]
            pair_copy(block, block, send_sem.at[0], half_recv.at[0]).start()

        if start == spare:
            pl.when(jnp.logical_not(gives))(push_half)
        else:
            push_half()

    def update_down(start, size, ratio):
        scale = jnp.broadcast_to(ratio, (ROWS, LANES))
        lanes = pl.ds(start, size)
        place = pl.ds(mine + start, size)

        per = down_per

        @pl.loop(0, depth // per)
        def _(p):
            @pl.loop(0, per // down_rows)
            def _(r):
                for q in range(down_rows // ROWS):
                    rows = pl.ds(p * per + r * down_rows + q * ROWS, ROWS)
                    new = next_down[rows, lanes] - sum_down(rows, lanes) * scale
                    next_down[rows, lanes] = new
                    half_down[rows, place] = new.astype(jnp.bfloat16)

            block = half_down.at[pl.ds(p * per, per), place]
            pair_copy(block, block, send_sem.at[0], half_recv.at[0]).start()

    def exchange(load_sem, early_send, slope_recv):
        loads = {}

        def load(name, source, target):
            copy = pltpu.make_async_copy(source, target, load_sem.at[len(loads)])
            copy.start()
            loads[name] = copy

        barrier = pltpu.get_barrier_semaphore()

        @pl.when(lead)
        def _():
            pl.semaphore_signal(
                barrier, inc=1, device_id={"replica": other}, device_id_type=MESH
            )

        @pl.when(jnp.logical_not(lead))
        def _():
            pl.semaphore_wait(barrier, 1)
            pl.semaphore_signal(
                pair_ready, inc=1, device_id={"replica": other}, device_id_type=MESH
            )

        first = {}
        parts = [("down", 0, LANES), ("down", LANES, share - LANES), ("up", 0, share)]
        for span in parts:
            if span[2]:
                load(
                    ("param", span),
                    cut(span[0], param_up, param_down, *span[1:]),
                    cut(span[0], next_up, next_down, *span[1:]),
                )
                load(
                    ("slope", span),
                    own_slope(*span),
                    cut(span[0], own_up, own_down, *span[1:]),
                )
                for piece_span in pieces:
                    if piece_span[0] == span[0] and piece_span[1] == span[1]:
                        first[piece_span] = span
        load("slope norm", slope_norm, own_vec)
        load("param norm", param_norm, own_gain)

        @pl.when(jnp.logical_and(spot == 0, lead))
        def _():
            pltpu.make_async_copy(
                peer_slope("up", spare, LANES), lent_own, lent_load.at[0]
            ).start()

        @pl.when(lead)
        def _():
            pl.semaphore_wait(pair_ready, 1)
            for k in range(1, models):
                pl.semaphore_signal(
                    barrier,
                    inc=1,
                    device_id={"model": lax.rem(spot + k, models)},
                    device_id_type=MESH,
                )

        def meet_models():
            @pl.when(lead)
            def _():
                pl.semaphore_wait(barrier, models - 1)
                pl.semaphore_signal(
                    model_ready, inc=1, device_id={"replica": other}, device_id_type=MESH
                )

            @pl.when(jnp.logical_not(lead))
            def _():
                pl.semaphore_wait(model_ready, 1)

        for n, span in enumerate(pieces):
            pair_copy(
                peer_slope(*span),
                cut(span[0], peer_up, peer_down, *span[1:]),
                early_send.at[0],
                slope_recv.at[n],
            ).start()
        norms = [
            pair_copy(slope_norm, peer_vec, early_send.at[1], slope_recv.at[len(pieces)]),
            pair_copy(param_norm, peer_gain, early_send.at[2], slope_recv.at[len(pieces) + 1]),
        ]
        for copy in norms:
            copy.start()

        @pl.when(gives)
        def _():
            for copy in lent:
                copy.start()

        def measure_piece(n):
            kind, start, size = pieces[n]
            squares = row_squares if kind == "up" else column_squares
            param = next_up if kind == "up" else next_down
            total = sum_up if kind == "up" else sum_down
            span = first.get(pieces[n])
            if span:
                loads["param", span].wait()
            piece[n, 0:1] = squares(start, size, lambda rows, lanes: param[rows, lanes])
            if span:
                loads["slope", span].wait()
            pair_copy(
                peer_slope(*pieces[n]),
                cut(kind, peer_up, peer_down, start, size),
                early_send.at[0],
                slope_recv.at[n],
            ).wait_recv()
            piece[n, 1:2] = squares(start, size, total)
            if n == 0:
                meet_models()
            share_norm(n)
            if n == last:

                @pl.when(jnp.logical_not(lead))
                def _():
                    lend_norm(piece.at[n], lent_norm.at[models - 1 - spot]).start()

        def update_norm():
            loads["slope norm"].wait()
            loads["param norm"].wait()
            for copy in norms:
                copy.wait_recv()
            sum_vec[...] = (
                (own_vec[...].astype(f32) + peer_vec[...].astype(f32)) * rate * learn_rate
            )
            new_gain = own_gain[...].reshape(1, share) - sum_vec[:, pl.ds(mine, share)]
            gain[:, pl.ds(mine, share)] = new_gain
            gain[:, pl.ds(theirs, share)] = (
                peer_gain[...].reshape(1, share) - sum_vec[:, pl.ds(theirs, share)]
            )
            next_norm[...] = new_gain.reshape(share)
            half_norm[...] = gain[...].reshape(half_norm.shape).astype(jnp.bfloat16)

        for n in range(len(pieces)):
            measure_piece(n)
        update_norm()
        pair_copy(half_up, half_up, early_send.at[0], slope_recv.at[0]).wait_send()
        for copy in norms:
            copy.wait_send()

    def begin(front_recv):
        scoped.append(front_recv)
        pl.run_scoped(
            exchange,
            load_sem=pltpu.SemaphoreType.DMA((8,)),
            early_send=pltpu.SemaphoreType.DMA((3,)),
            slope_recv=pltpu.SemaphoreType.DMA((len(pieces) + 2,)),
        )
        for n in range(front):
            update_piece(n)
        scoped.clear()

    pl.run_scoped(begin, front_recv=pltpu.SemaphoreType.DMA((front,)))
    for n in range(front, len(pieces)):
        update_piece(n)

    @pl.when(takes)
    def _():
        lent_both.wait_recv()
        pltpu.make_async_copy(
            peer_slope("up", spare, LANES), lent_own, lent_load.at[0]
        ).wait()
        lend_norm(lent_norm, lent_norm).wait_recv()
        whole = lent_norm[models - 1]
        for k in range(1, models):
            whole = whole + lent_norm[k - 1]
        spread[...] = jnp.broadcast_to(ratio_of(whole), (LANES, LANES)).T

        @pl.loop(0, LANES // ROWS)
        def _(r):
            rows = pl.ds(r * ROWS, ROWS)
            scale = spread[rows, :]
            for j in range(inner // LANES):
                lanes = pl.ds(j * LANES, LANES)
                total = lent_slope[rows, lanes].astype(f32) + lent_own[
                    rows, lanes
                ].astype(f32)
                half_up[pl.ds(theirs + spare + r * ROWS, ROWS), lanes] = (
                    lent_param[rows, lanes] - total * scale
                ).astype(jnp.bfloat16)

    def halves(rows):
        block = half_up.at[pl.ds(0, rows), :]
        return pair_copy(block, block, send_sem.at[0], half_recv.at[0])

    @pl.when(gives)
    def _():
        halves(2 * share - LANES).wait_send()
        lent_both.wait_send()

    @pl.when(jnp.logical_not(gives))
    def _():
        halves(2 * share).wait_send()

    @pl.when(takes)
    def _():
        halves(2 * share - LANES).wait_recv()

    @pl.when(jnp.logical_not(takes))
    def _():
        halves(2 * share).wait_recv()

    @pl.when(jnp.logical_not(lead))
    def _():
        lend_norm(piece.at[last], lent_norm.at[0]).wait_send()

    norm_copy(got_piece, got_piece, 0, 1).wait_send()


def steps_of(depth):
    cuts = max(c for c in range(1, DOWN_CUTS + 1) if depth % (c * ROWS) == 0)
    per = depth // cuts
    return per, max(k * ROWS for k in range(1, 11) if per % (k * ROWS) == 0)


def pieces_of(share):
    pieces = [("down", start, LANES) for start in range(0, share, LANES)]
    pieces += [("up", start, LANES) for start in range(0, share, LANES)]
    return pieces


def write_kernel(
    half_up,
    half_down,
    half_norm,
    next_up,
    next_down,
    next_norm,
    half_up_out,
    half_down_out,
    half_norm_out,
    next_up_out,
    next_down_out,
    next_norm_out,
    sem,
):
    moves = (
        (half_norm, half_norm_out),
        (next_norm, next_norm_out),
        (half_up, half_up_out),
        (half_down, half_down_out),
        (next_up, next_up_out),
        (next_down, next_down_out),
    )
    for i, (source, target) in enumerate(moves):
        cuts = 8 if len(source.shape) == 2 else 1
        rows = source.shape[0] // cuts
        for c in range(cuts):
            part = pl.ds(c * rows, rows)
            pltpu.make_async_copy(source.at[part], target.at[part], sem.at[i]).start()
    for i, (source, target) in enumerate(moves):
        pltpu.make_async_copy(source, target, sem.at[i]).wait()


def fused(replicas, models, slope_up, slope_down, slope_norm, param_up, param_down, param_norm):
    share, inner = param_up.shape
    depth = param_down.shape[0]
    width = slope_up.shape[1]
    count = len(pieces_of(share))
    bf16, f32 = jnp.bfloat16, jnp.float32
    hbm = pl.BlockSpec(memory_space=pltpu.HBM)
    vmem = pl.BlockSpec(memory_space=pltpu.VMEM)
    outs = pl.pallas_call(
        functools.partial(update_kernel, replicas, models),
        out_shape=(
            OUT((width, inner), bf16),
            OUT((depth, width), bf16),
            OUT((width,), bf16),
            OUT((share, inner), f32),
            OUT((depth, share), f32),
            OUT((share,), f32),
        ),
        in_specs=[hbm] * 6,
        out_specs=(vmem,) * 6,
        scratch_shapes=[
            pltpu.VMEM((share, inner), bf16),
            pltpu.VMEM((share, inner), bf16),
            pltpu.VMEM((depth, share), bf16),
            pltpu.VMEM((depth, share), bf16),
            pltpu.VMEM((1, width), bf16),
            pltpu.VMEM((1, width), bf16),
            pltpu.VMEM((share,), f32),
            pltpu.VMEM((share,), f32),
            pltpu.VMEM((1, width), f32),
            pltpu.VMEM((1, width), f32),
            pltpu.VMEM((LANES, inner), f32),
            pltpu.VMEM((LANES, inner), bf16),
            pltpu.VMEM((LANES, inner), bf16),
            pltpu.VMEM((models, 2, LANES), f32),
            pltpu.VMEM((count, 2, LANES), f32),
            pltpu.VMEM((count, models - 1, 2, LANES), f32),
            pltpu.VMEM((LANES, LANES), f32),
            pltpu.VMEM((LANES, LANES), f32),
            pltpu.SemaphoreType.DMA((1,)),
            pltpu.SemaphoreType.DMA((4,)),
            pltpu.SemaphoreType.DMA((1,)),
            pltpu.SemaphoreType.DMA((3,)),
            pltpu.SemaphoreType.DMA((2,)),
            pltpu.SemaphoreType.REGULAR,
            pltpu.SemaphoreType.REGULAR,
        ],
        compiler_params=pltpu.CompilerParams(
            collective_id=0, has_side_effects=True, vmem_limit_bytes=24 * 2**20
        ),
    )(
        *(
            pltpu.with_memory_space_constraint(x, pltpu.HBM)
            for x in (
                slope_up, slope_down, slope_norm, param_up, param_down, param_norm
            )
        )
    )
    return pl.pallas_call(
        write_kernel,
        out_shape=(
            jax.ShapeDtypeStruct((width, inner), bf16),
            jax.ShapeDtypeStruct((depth, width), bf16),
            jax.ShapeDtypeStruct((width,), bf16),
            jax.ShapeDtypeStruct((share, inner), f32),
            jax.ShapeDtypeStruct((depth, share), f32),
            jax.ShapeDtypeStruct((share,), f32),
        ),
        in_specs=[vmem] * 6,
        out_specs=(hbm,) * 6,
        scratch_shapes=[pltpu.SemaphoreType.DMA((6,))],
        compiler_params=pltpu.CompilerParams(vmem_limit_bytes=24 * 2**20),
    )(*(pltpu.with_memory_space_constraint(x, pltpu.VMEM) for x in outs))


def suits(mesh, *arrays):
    slope_up, param_up, param_down = arrays
    return (
        mesh.shape["replica"] == 2
        and mesh.shape["model"] > 1
        and param_up.shape[0] % LANES == 0
        and param_up.shape[0] > LANES
        and param_up.shape[1] == param_down.shape[0]
        and param_down.shape[1] == param_up.shape[0]
        and param_up.shape[1] % LANES == 0
        and param_down.shape[0] % LANES == 0
    )


def step(mesh, slope_up, slope_down, slope_norm, param_up, param_down, param_norm):
    args = (slope_up, slope_down, slope_norm, param_up, param_down, param_norm)
    if suits(mesh, slope_up, param_up, param_down):
        return fused(mesh.shape["replica"], mesh.shape["model"], *args)
    return shards(*args)


OUT = pltpu.VMEM


def solution(mesh):
    return jax.shard_map(
        functools.partial(step, mesh),
        mesh=mesh,
        in_specs=(
            P(("copy", "replica"), None, "model"),
            P(("copy", "replica"), "model", None),
            P(("copy", "replica"), None),
            P(("copy", "replica"), "model"),
            P(("copy", "model"), "replica"),
            P(("copy", "replica")),
        ),
        out_specs=(
            P("copy", "model"),
            P(("copy", "model"), None),
            P("copy"),
            P(("copy", "replica"), "model"),
            P(("copy", "model"), "replica"),
            P(("copy", "replica")),
        ),
        check_vma=False,
    )
```
